16 devices in a mesh: dp: 4 (over z, y), tp: 4 (over x, core).
Axes of the slice: x: 2, y: 2, z: 2, core: 2. Of those that a mesh axis runs over, the one named last changes fastest.
Arguments:
- resid_in: bfloat16 [1024, 2048], P('dp'), parts along dimension 0
- positions: int32 [1024], P('dp'), parts along dimension 0
- k_cache: bfloat16 [1024, 256, 8, 64], P('dp', None, 'tp'), parts along dimension 0
- v_cache: bfloat16 [1024, 256, 8, 64], P('dp', None, 'tp'), parts along dimension 0
- gain_attn: bfloat16 [2048], replicated
- w_query: bfloat16 [2048, 2048], P(None, 'tp')
- w_key: bfloat16 [2048, 512], P(None, 'tp')
- w_value: bfloat16 [2048, 512], P(None, 'tp')
- w_out: bfloat16 [2048, 2048], P('tp')
- gain_mlp: bfloat16 [2048], replicated
- w_gate: bfloat16 [2048, 8192], P(None, 'tp')
- w_up: bfloat16 [2048, 8192], P(None, 'tp')
- w_down: bfloat16 [8192, 2048], P('tp')
Outputs:
- output 1: bfloat16 [1024, 2048], P('dp'), parts along dimension 0
- output 2: bfloat16 [1024, 256, 8, 64], P('dp', None, 'tp'), parts along dimension 0
- output 3: bfloat16 [1024, 256, 8, 64], P('dp', None, 'tp'), parts along dimension 0
There are 4 independent parts. The reference program is written for one: setup_inputs(seed, part) draws one part's arguments, and reference() takes and returns one part's arrays. A program takes and returns all parts, laid end to end along the dimension named above; an argument that names none is the same for every part.
All inputs are finite; a program needn't handle non-finite values.
Results may differ from the reference program's by a relative error of at most 0.0103436.
Values sent between devices are 32-bit elements.
A program may use at most 1 GiB of HBM per device.

```python
import math
import jax
import jax.numpy as jnp
from jax import lax

BATCH_PART = 256
CACHE_LEN = 256
MODEL_DIM = 2048
Q_HEADS = 32
KV_HEADS = 8
HEAD_DIM = 64
FFN_DIM = 8192

EPS = 1e-5
ROPE_THETA = 500000.0
ROPE_FACTOR = 8.0
LOW_FACTOR = 1.0
HIGH_FACTOR = 4.0
ORIG_CTX = 8192.0


def setup_inputs(seed: int = 0, part: int = 0) -> dict:
    part_keys = jax.random.split(jax.random.fold_in(jax.random.key(seed), part), 6)
    weight_keys = jax.random.split(jax.random.key(seed + 1), 11)
    log_len = int(math.log2(CACHE_LEN))
    dim_scale = 1.0 / math.sqrt(MODEL_DIM)
    out_scale = 1.0 / math.sqrt(Q_HEADS * HEAD_DIM)
    ffn_scale = 1.0 / math.sqrt(FFN_DIM)
    q_width = Q_HEADS * HEAD_DIM
    kv_width = KV_HEADS * HEAD_DIM
    resid_in = jax.random.normal(part_keys[0], (BATCH_PART, MODEL_DIM), jnp.float32)
    exponent = jax.random.randint(part_keys[1], (BATCH_PART,), 0, log_len + 1, dtype=jnp.int32)
    upper_bound = jnp.left_shift(jnp.ones((BATCH_PART,), jnp.int32), exponent)
    positions = jax.random.randint(part_keys[2], (BATCH_PART,), 0, upper_bound, dtype=jnp.int32)
    positions = positions.at[0].set(CACHE_LEN - 1).at[1].set(0)
    cache_shape = (BATCH_PART, CACHE_LEN, KV_HEADS, HEAD_DIM)
    k_cache = jax.random.normal(part_keys[3], cache_shape, jnp.float32)
    v_mean = 0.7 * jax.random.normal(part_keys[4], (BATCH_PART, 1, KV_HEADS, HEAD_DIM), jnp.float32)
    v_cache = v_mean + jax.random.normal(part_keys[5], cache_shape, jnp.float32)
    gain_attn = 1.0 + 0.3 * jax.random.normal(weight_keys[0], (MODEL_DIM,), jnp.float32)
    w_query = jax.random.normal(weight_keys[1], (MODEL_DIM, q_width), jnp.float32) * dim_scale
    w_key = jax.random.normal(weight_keys[2], (MODEL_DIM, kv_width), jnp.float32) * dim_scale
    w_value = jax.random.normal(weight_keys[3], (MODEL_DIM, kv_width), jnp.float32) * dim_scale
    w_out = jax.random.normal(weight_keys[4], (q_width, MODEL_DIM), jnp.float32) * out_scale
    gain_mlp = 1.0 + 0.3 * jax.random.normal(weight_keys[5], (MODEL_DIM,), jnp.float32)
    w_gate = jax.random.normal(weight_keys[6], (MODEL_DIM, FFN_DIM), jnp.float32) * dim_scale
    w_up = jax.random.normal(weight_keys[7], (MODEL_DIM, FFN_DIM), jnp.float32) * dim_scale
    w_down = jax.random.normal(weight_keys[8], (FFN_DIM, MODEL_DIM), jnp.float32) * ffn_scale
    return dict(resid_in=resid_in.astype(jnp.bfloat16), positions=positions,
                k_cache=k_cache.astype(jnp.bfloat16), v_cache=v_cache.astype(jnp.bfloat16),
                gain_attn=gain_attn.astype(jnp.bfloat16), w_query=w_query.astype(jnp.bfloat16),
                w_key=w_key.astype(jnp.bfloat16), w_value=w_value.astype(jnp.bfloat16),
                w_out=w_out.astype(jnp.bfloat16), gain_mlp=gain_mlp.astype(jnp.bfloat16),
                w_gate=w_gate.astype(jnp.bfloat16), w_up=w_up.astype(jnp.bfloat16),
                w_down=w_down.astype(jnp.bfloat16))


def rms_norm(rows_in, gain):
    rows_f = rows_in.astype(jnp.float32)
    mean_sq = jnp.mean(rows_f * rows_f, axis=-1, keepdims=True)
    return (rows_f * lax.rsqrt(mean_sq + EPS) * gain.astype(jnp.float32)).astype(jnp.bfloat16)


def rope_tables(positions, head_dim):
    half_dim = head_dim // 2
    exponents = jnp.arange(half_dim, dtype=jnp.float32) * (2.0 / head_dim)
    inv_freq = 1.0 / jnp.power(ROPE_THETA, exponents)
    wavelen = (2.0 * math.pi) / inv_freq
    smooth = (ORIG_CTX / wavelen - LOW_FACTOR) / (HIGH_FACTOR - LOW_FACTOR)
    blended = (1.0 - smooth) * inv_freq / ROPE_FACTOR + smooth * inv_freq
    inv_freq = jnp.where(wavelen < ORIG_CTX / HIGH_FACTOR, inv_freq,
                         jnp.where(wavelen > ORIG_CTX / LOW_FACTOR, inv_freq / ROPE_FACTOR, blended))
    angles = positions.astype(jnp.float32)[:, None] * inv_freq[None, :]
    return jnp.cos(angles), jnp.sin(angles)


def apply_rope(vectors, cos_t, sin_t):
    half_dim = vectors.shape[-1] // 2
    lower_half = vectors[..., :half_dim]
    upper_half = vectors[..., half_dim:]
    cos_b = cos_t[:, None, :]
    sin_b = sin_t[:, None, :]
    return jnp.concatenate([lower_half * cos_b - upper_half * sin_b,
                            upper_half * cos_b + lower_half * sin_b], axis=-1)


def reference(resid_in, positions, k_cache, v_cache, gain_attn, w_query, w_key, w_value,
              w_out, gain_mlp, w_gate, w_up, w_down):
    group_size = Q_HEADS // KV_HEADS
    n_seqs = resid_in.shape[0]
    normed = rms_norm(resid_in, gain_attn)
    queries = jnp.dot(normed, w_query, preferred_element_type=jnp.float32).astype(jnp.bfloat16)
    key_new = jnp.dot(normed, w_key, preferred_element_type=jnp.float32).astype(jnp.bfloat16)
    value_new = jnp.dot(normed, w_value, preferred_element_type=jnp.float32).astype(jnp.bfloat16)
    cos_t, sin_t = rope_tables(positions, HEAD_DIM)
    queries = apply_rope(queries.reshape(n_seqs, Q_HEADS, HEAD_DIM).astype(jnp.float32), cos_t, sin_t)
    queries = queries.astype(jnp.bfloat16)
    key_new = apply_rope(key_new.reshape(n_seqs, KV_HEADS, HEAD_DIM).astype(jnp.float32), cos_t, sin_t)
    key_new = key_new.astype(jnp.bfloat16)
    value_new = value_new.reshape(n_seqs, KV_HEADS, HEAD_DIM)
    slot_hit = (jnp.arange(CACHE_LEN)[None, :] == positions[:, None])[:, :, None, None]
    k_full = jnp.where(slot_hit, key_new[:, None], k_cache)
    v_full = jnp.where(slot_hit, value_new[:, None], v_cache)
    scale = 1.0 / math.sqrt(HEAD_DIM)

    def one_seq(seq_items):
        q_seq, k_seq, v_seq, pos_seq = seq_items
        q_grp = q_seq.reshape(KV_HEADS, group_size, HEAD_DIM).astype(jnp.float32)
        scores = jnp.einsum('kgd,skd->kgs', q_grp, k_seq.astype(jnp.float32)) * scale
        valid = jnp.arange(CACHE_LEN) <= pos_seq
        scores = jnp.where(valid[None, None, :], scores, -jnp.inf)
        attn_prob = jax.nn.softmax(scores, axis=-1).astype(jnp.bfloat16)
        attn_seq = jnp.einsum('kgs,skd->kgd', attn_prob.astype(jnp.float32), v_seq.astype(jnp.float32))
        return attn_seq.astype(jnp.bfloat16).reshape(Q_HEADS * HEAD_DIM)

    attn_out = lax.map(one_seq, (queries, k_full, v_full, positions))
    y_full = jnp.dot(attn_out, w_out, preferred_element_type=jnp.float32)
    resid_mid = (resid_in.astype(jnp.float32) + y_full).astype(jnp.bfloat16)
    normed_mlp = rms_norm(resid_mid, gain_mlp)
    gate_proj = jnp.dot(normed_mlp, w_gate, preferred_element_type=jnp.float32).astype(jnp.bfloat16)
    up_proj = jnp.dot(normed_mlp, w_up, preferred_element_type=jnp.float32).astype(jnp.bfloat16)
    hidden = (jax.nn.silu(gate_proj.astype(jnp.float32)) * up_proj.astype(jnp.float32)).astype(jnp.bfloat16)
    z_full = jnp.dot(hidden, w_down, preferred_element_type=jnp.float32)
    resid_out = (resid_mid.astype(jnp.float32) + z_full).astype(jnp.bfloat16)
    return resid_out, k_full, v_full
```

```python
import functools
import math
import numpy as np
import jax
import jax.numpy as jnp
from jax import lax
from jax.experimental import pallas as pl
from jax.experimental.pallas import tpu as pltpu
from jax.sharding import PartitionSpec as P

EPS = 1e-5
ROPE_THETA = 500000.0
ROPE_FACTOR = 8.0
LOW_FACTOR = 1.0
HIGH_FACTOR = 4.0
ORIG_CTX = 8192.0
MESH = pl.DeviceIdType.MESH
F32 = jnp.float32
BF16 = jnp.bfloat16

HEAD = 64
PAIR = 128
GROUP = 4
SEQS = 16
SUB = 8


def frequency_lanes():
    half = HEAD // 2
    exponents = np.arange(half, dtype=np.float32) * np.float32(2.0 / HEAD)
    inv_freq = (1.0 / np.power(np.float32(ROPE_THETA), exponents)).astype(np.float32)
    wavelen = (2.0 * math.pi) / inv_freq
    smooth = (ORIG_CTX / wavelen - LOW_FACTOR) / (HIGH_FACTOR - LOW_FACTOR)
    blended = (1.0 - smooth) * inv_freq / ROPE_FACTOR + smooth * inv_freq
    inv_freq = np.where(wavelen < ORIG_CTX / HIGH_FACTOR, inv_freq,
                        np.where(wavelen > ORIG_CTX / LOW_FACTOR, inv_freq / ROPE_FACTOR, blended))
    lanes = np.arange(PAIR)
    freq = inv_freq[lanes % half].astype(np.float32)
    sign = np.where(lanes % HEAD < half, -1.0, 1.0).astype(np.float32)
    return np.stack([freq, sign])


def attention_kernel(pos_smem, pos_row, freq_ref, resid_ref, gain_ref, wq_ref, wk_ref, wv_ref, kc_ref, vc_ref,
                     o_ref, ko_ref, vo_ref, h_scr, q_scr, k_scr, v_scr, pos_scr):
    step = pl.program_id(0)
    n_seqs, dim = resid_ref.shape
    cache_len = kc_ref.shape[1]

    @pl.when(step == 0)
    def _project():
        rows = 64
        for i in range(n_seqs // rows):
            x = resid_ref[i * rows:(i + 1) * rows, :].astype(F32)
            mean_sq = jnp.sum(x * x, axis=1, keepdims=True) * (1.0 / dim)
            h_scr[i * rows:(i + 1) * rows, :] = (x * lax.rsqrt(mean_sq + EPS) * gain_ref[...].astype(F32)).astype(BF16)
        diag = (lax.broadcasted_iota(jnp.int32, (n_seqs, n_seqs), 0)
                == lax.broadcasted_iota(jnp.int32, (n_seqs, n_seqs), 1))
        pos_col = jnp.sum(jnp.where(diag, pos_row[...].astype(F32), 0.0), axis=1, keepdims=True)
        pos_scr[...] = jnp.broadcast_to(pos_col, (n_seqs, PAIR))
        angles = pos_scr[...] * freq_ref[0:1, :]
        cos_t = jnp.cos(angles)
        sin_t = jnp.sin(angles) * freq_ref[1:2, :]
        lane = lax.broadcasted_iota(jnp.int32, (n_seqs, PAIR), 1)
        low = lane % HEAD < HEAD // 2
        first = lane < HEAD

        def rope(t):
            t = t.astype(BF16).astype(F32)
            swapped = jnp.where(low, pltpu.roll(t, PAIR - HEAD // 2, 1), pltpu.roll(t, HEAD // 2, 1))
            return (t * cos_t + swapped * sin_t).astype(BF16).astype(F32)

        h = h_scr[...]
        tiles = [rope(jnp.dot(h, wq_ref[:, t * PAIR:(t + 1) * PAIR], preferred_element_type=F32)) for t in range(GROUP)]
        for g in range(GROUP):
            lower, upper = tiles[g // 2], tiles[2 + g // 2]
            if g % 2 == 0:
                upper = pltpu.roll(upper, HEAD, 1)
            else:
                lower = pltpu.roll(lower, HEAD, 1)
            q_scr[g, :, :] = jnp.where(first, lower, upper)
        k_scr[...] = rope(jnp.dot(h, wk_ref[...], preferred_element_type=F32))
        v_scr[...] = jnp.dot(h, wv_ref[...], preferred_element_type=F32).astype(BF16).astype(F32)

    lane_s = lax.broadcasted_iota(jnp.int32, (PAIR, cache_len), 1)
    lane_q = lax.broadcasted_iota(jnp.int32, (SUB, PAIR), 1)
    sub_q = lax.broadcasted_iota(jnp.int32, (SUB, PAIR), 0)
    head_mask = [lane_q < HEAD, lane_q >= HEAD]
    lane_p = lax.broadcasted_iota(jnp.int32, (SUB, cache_len), 1)
    o_parts = [[] for _ in range(GROUP)]
    for t in range(SEQS // SUB):
        base = pl.multiple_of(step * SEQS + t * SUB, SUB)
        k_t = k_scr[pl.ds(base, SUB), :].T
        v_t = v_scr[pl.ds(base, SUB), :].T
        for b in range(SUB):
            hit = lane_s == pos_smem[base + b]
            lo = (t * SUB + b) * PAIR
            ko_ref[lo:lo + PAIR, :] = jnp.where(hit, k_t[:, b:b + 1], kc_ref[lo:lo + PAIR, :].astype(F32)).astype(BF16)
            vo_ref[lo:lo + PAIR, :] = jnp.where(hit, v_t[:, b:b + 1], vc_ref[lo:lo + PAIR, :].astype(F32)).astype(BF16)
        lo = t * SUB * PAIR
        k_blk = ko_ref[lo:lo + SUB * PAIR, :]
        v_blk = vo_ref[lo:lo + SUB * PAIR, :]
        q_rows = []
        for g in range(GROUP):
            q_g = q_scr[g, pl.ds(base, SUB), :]
            for h in range(2):
                q_h = jnp.where(head_mask[h], q_g, 0.0)
                q_rows.append(jnp.concatenate([jnp.where(sub_q == b, q_h, 0.0) for b in range(SUB)], axis=1))
        q_bd = jnp.concatenate(q_rows, axis=0).astype(BF16)
        scores = jnp.dot(q_bd, k_blk, preferred_element_type=F32) * (1.0 / math.sqrt(HEAD))
        pos8 = pos_scr[pl.ds(base, SUB), 0:1].astype(jnp.int32)
        valid = lane_p <= pos8
        scores = jnp.where(jnp.concatenate([valid] * (2 * GROUP), axis=0), scores, -jnp.inf)
        top = jnp.max(scores, axis=1, keepdims=True)
        expd = jnp.exp(scores - top)
        prob = (expd / jnp.sum(expd, axis=1, keepdims=True)).astype(BF16)
        mixed = lax.dot_general(prob, v_blk, (((1,), (1,)), ((), ())), preferred_element_type=F32)
        for g in range(GROUP):
            acc = None
            for h in range(2):
                r = (g * 2 + h) * SUB
                part = mixed[r:r + SUB, 0:PAIR]
                for b in range(1, SUB):
                    part = jnp.where(sub_q == b, mixed[r:r + SUB, b * PAIR:(b + 1) * PAIR], part)
                acc = part if acc is None else jnp.where(head_mask[1], part, acc)
            o_parts[g].append(acc)
    for g in range(GROUP):
        o_ref[:, g * PAIR:(g + 1) * PAIR] = jnp.concatenate(o_parts[g], axis=0).astype(BF16)


def attention_call(resid_in, positions, kc, vc, gain, w_query, w_key, w_value):
    n_seqs, dim = resid_in.shape
    cache_len = kc.shape[1]
    rows = SEQS * PAIR
    whole = lambda shape: pl.BlockSpec(shape, lambda i, p: (0,) * len(shape))
    cache_spec = pl.BlockSpec((rows, cache_len), lambda i, p: (i, 0))
    freq = jnp.asarray(frequency_lanes())
    return pl.pallas_call(
        attention_kernel,
        out_shape=(jax.ShapeDtypeStruct((n_seqs, 2 * GROUP * HEAD), BF16),
                   jax.ShapeDtypeStruct(kc.shape, BF16), jax.ShapeDtypeStruct(vc.shape, BF16)),
        grid_spec=pltpu.PrefetchScalarGridSpec(
            num_scalar_prefetch=1, grid=(n_seqs // SEQS,),
            in_specs=[whole((1, n_seqs)), whole((2, PAIR)), whole((n_seqs, dim)), whole((1, dim)), whole(w_query.shape),
                      whole(w_key.shape), whole(w_value.shape), cache_spec, cache_spec],
            out_specs=(pl.BlockSpec((SEQS, 2 * GROUP * HEAD), lambda i, p: (i, 0)), cache_spec, cache_spec),
            scratch_shapes=[pltpu.VMEM((n_seqs, dim), BF16), pltpu.VMEM((GROUP, n_seqs, PAIR), F32),
                            pltpu.VMEM((n_seqs, PAIR), F32), pltpu.VMEM((n_seqs, PAIR), F32),
                            pltpu.VMEM((n_seqs, PAIR), F32)]),
        compiler_params=pltpu.CompilerParams(dimension_semantics=("arbitrary",), vmem_limit_bytes=48 << 20),
        name="attention",
    )(positions, positions.reshape(1, n_seqs), freq, resid_in, gain.reshape(1, dim), w_query, w_key, w_value, kc, vc)


N_CHUNK = 4
N_HALF = 2


def mlp_kernel(o_ref, resid_ref, gain_ref, wo_hbm, wg_hbm, wu_hbm, wd_hbm, out_ref,
               wo_v, wg_v, wu_v, wd_v, part, near, mine, far, full, h_scr, a_scr,
               wo_sem, w_sem, near_send, near_recv, far_send, far_recv, back_send, back_recv):
    tp = lax.axis_index("tp")
    dp = lax.axis_index("dp")
    core = lax.rem(tp, 2)
    other = 1 - core
    sibling = tp + 1 - 2 * core
    partner = lax.rem(tp + 2, 4)
    n_seqs = o_ref.shape[0]
    half_dim = resid_ref.shape[1] // 2
    ffn = wg_v.shape[1]
    rows = n_seqs // N_CHUNK

    wo_copies = []
    for g in range(GROUP):
        for h in range(2):
            for s in range(2):
                wo_copies.append(pltpu.make_async_copy(
                    wo_hbm.at[pl.ds((h * GROUP + g) * HEAD, HEAD), pl.ds(s * half_dim, half_dim)],
                    wo_v.at[s, pl.ds((2 * g + h) * HEAD, HEAD), :], wo_sem.at[(2 * g + h) * 2 + s]))
    for c in wo_copies:
        c.start()
    w_copies = [pltpu.make_async_copy(src, dst, w_sem.at[i])
                for i, (src, dst) in enumerate(((wg_hbm, wg_v), (wu_hbm, wu_v), (wd_hbm, wd_v)))]
    for c in w_copies:
        c.start()

    barrier = pltpu.get_barrier_semaphore()
    for peer in (sibling, partner):
        pl.semaphore_signal(barrier, inc=1, device_id=(dp, peer), device_id_type=MESH)
    pl.semaphore_wait(barrier, 2)

    def remote(src, dst, sems, k, r, peer):
        return pltpu.make_async_remote_copy(src_ref=src, dst_ref=dst, send_sem=sems[0].at[k, r], recv_sem=sems[1].at[k, r],
                                            device_id=(dp, peer), device_id_type=MESH)

    def chunk(r):
        return pl.ds(r * rows, rows)

    def near_copy(k, r):
        return remote(part.at[k, other, chunk(r)], near.at[k, chunk(r)], (near_send, near_recv), k, r, sibling)

    def far_copy(k, r):
        return remote(mine.at[k, chunk(r)], far.at[k, chunk(r)], (far_send, far_recv), k, r, partner)

    def back_copy(k, r):
        return remote(full.at[k, core, chunk(r)], full.at[k, core, chunk(r)], (back_send, back_recv), k, r, sibling)

    def sum_near(k, r):
        near_copy(k, r).wait_recv()
        mine[k, chunk(r), :] = part[k, core, chunk(r), :] + near[k, chunk(r), :]
        far_copy(k, r).start()

    my_cols = pl.ds(pl.multiple_of(core * half_dim, half_dim), half_dim)
    other_cols = pl.ds(pl.multiple_of(other * half_dim, half_dim), half_dim)

    def sum_far_y(r):
        far_copy(0, r).wait_recv()
        total = resid_ref[chunk(r), my_cols].astype(F32) + (mine[0, chunk(r), :] + far[0, chunk(r), :])
        full[0, core, chunk(r), :] = total.astype(BF16).astype(F32)
        back_copy(0, r).start()

    def sum_far_z(r):
        far_copy(1, r).wait_recv()
        total = full[0, core, chunk(r), :] + (mine[1, chunk(r), :] + far[1, chunk(r), :])
        rounded = total.astype(BF16)
        full[1, core, chunk(r), :] = rounded.astype(F32)
        back_copy(1, r).start()
        out_ref[chunk(r), my_cols] = rounded

    for c in wo_copies:
        c.wait()
    for r in range(N_CHUNK):
        o = o_ref[chunk(r), :]
        part[0, other, chunk(r), :] = jnp.dot(o, wo_v[other], preferred_element_type=F32)
        near_copy(0, r).start()
        part[0, core, chunk(r), :] = jnp.dot(o, wo_v[core], preferred_element_type=F32)
        if r > 0:
            sum_near(0, r - 1)
    sum_near(0, N_CHUNK - 1)

    tile = 512
    per_half = N_CHUNK // N_HALF
    half_rows = n_seqs // N_HALF
    for m in range(N_HALF):
        for r in range(m * per_half, (m + 1) * per_half):
            sum_far_y(r)
        for r in range(m * per_half, (m + 1) * per_half):
            back_copy(0, r).wait_recv()
        for r in range(m * per_half, (m + 1) * per_half):
            x0 = full[0, 0, chunk(r), :]
            x1 = full[0, 1, chunk(r), :]
            mean_sq = (jnp.sum(x0 * x0, axis=1, keepdims=True)
                       + jnp.sum(x1 * x1, axis=1, keepdims=True)) * (0.5 / half_dim)
            inv = lax.rsqrt(mean_sq + EPS)
            at = pl.ds((r - m * per_half) * rows, rows)
            h_scr[at, :half_dim] = (x0 * inv * gain_ref[:, :half_dim].astype(F32)).astype(BF16)
            h_scr[at, half_dim:] = (x1 * inv * gain_ref[:, half_dim:].astype(F32)).astype(BF16)
        if m == 0:
            w_copies[0].wait()
            w_copies[1].wait()

        def up_tile(n, carry):
            cols = pl.ds(pl.multiple_of(n * tile, tile), tile)
            gate = jnp.dot(h_scr[...], wg_v[:, cols], preferred_element_type=F32).astype(BF16).astype(F32)
            up = jnp.dot(h_scr[...], wu_v[:, cols], preferred_element_type=F32).astype(BF16).astype(F32)
            a_scr[:, cols] = (gate * jax.nn.sigmoid(gate) * up).astype(BF16)
            return carry

        lax.fori_loop(0, ffn // tile, up_tile, 0)
        if m == 0:
            w_copies[2].wait()
        half_at = pl.ds(m * half_rows, half_rows)
        for s in (other, core):
            def down_tile(n, carry, s=s):
                cols = pl.ds(pl.multiple_of(s * half_dim + n * tile, tile), tile)
                part[1, s, half_at, pl.ds(pl.multiple_of(n * tile, tile), tile)] = jnp.dot(
                    a_scr[...], wd_v[:, cols], preferred_element_type=F32)
                return carry

            lax.fori_loop(0, half_dim // tile, down_tile, 0)
            if s is other:
                for r in range(m * per_half, (m + 1) * per_half):
                    near_copy(1, r).start()
        for r in range(m * per_half, (m + 1) * per_half):
            sum_near(1, r)

    for r in range(N_CHUNK):
        sum_far_z(r)
        if r > 0:
            back_copy(1, r - 1).wait_recv()
            out_ref[chunk(r - 1), other_cols] = full[1, other, chunk(r - 1), :].astype(BF16)
    back_copy(1, N_CHUNK - 1).wait_recv()
    out_ref[chunk(N_CHUNK - 1), other_cols] = full[1, other, chunk(N_CHUNK - 1), :].astype(BF16)
    for k in range(2):
        for r in range(N_CHUNK):
            near_copy(k, r).wait_send()
            far_copy(k, r).wait_send()
            back_copy(k, r).wait_send()


def mlp_call(o, resid_in, gain, w_out, w_gate, w_up, w_down):
    n_seqs, dim = resid_in.shape
    half = dim // 2
    ffn = w_gate.shape[1]
    vmem = pl.BlockSpec(memory_space=pltpu.VMEM)
    hbm = pl.BlockSpec(memory_space=pl.ANY)
    sems = pltpu.SemaphoreType.DMA((2, N_CHUNK))
    return pl.pallas_call(
        mlp_kernel,
        out_shape=jax.ShapeDtypeStruct((n_seqs, dim), BF16),
        in_specs=[vmem, vmem, vmem, hbm, hbm, hbm, hbm],
        out_specs=vmem,
        scratch_shapes=[
            pltpu.VMEM((2, w_out.shape[0], half), BF16), pltpu.VMEM(w_gate.shape, BF16),
            pltpu.VMEM(w_up.shape, BF16), pltpu.VMEM(w_down.shape, BF16),
            pltpu.VMEM((2, 2, n_seqs, half), F32), pltpu.VMEM((2, n_seqs, half), F32),
            pltpu.VMEM((2, n_seqs, half), F32), pltpu.VMEM((2, n_seqs, half), F32),
            pltpu.VMEM((2, 2, n_seqs, half), F32),
            pltpu.VMEM((n_seqs // N_HALF, dim), BF16), pltpu.VMEM((n_seqs // N_HALF, ffn), BF16),
            pltpu.SemaphoreType.DMA((16,)), pltpu.SemaphoreType.DMA((3,)),
            sems, sems, sems, sems, sems, sems],
        compiler_params=pltpu.CompilerParams(collective_id=0, has_side_effects=True, vmem_limit_bytes=60 << 20),
        name="mlp",
    )(o, resid_in, gain.reshape(1, dim), w_out, w_gate, w_up, w_down)


def solution(mesh):
    def layer_local(resid_in, positions, k_cache, v_cache, gain_attn, w_query, w_key, w_value,
                    w_out, gain_mlp, w_gate, w_up, w_down):
        n_seqs, cache_len, heads, dim = k_cache.shape
        flat = lambda c: jnp.transpose(c, (0, 2, 3, 1)).reshape(n_seqs * heads * dim, cache_len)
        back = lambda c: jnp.transpose(c.reshape(n_seqs, heads, dim, cache_len), (0, 3, 1, 2))
        o, k_full, v_full = attention_call(resid_in, positions, flat(k_cache), flat(v_cache),
                                           gain_attn, w_query, w_key, w_value)
        resid_out = mlp_call(o, resid_in, gain_mlp, w_out, w_gate, w_up, w_down)
        return resid_out, back(k_full), back(v_full)

    row_spec = P('dp', None)
    cache_spec = P('dp', None, 'tp', None)
    col_spec = P(None, 'tp')
    split_rows = P('tp', None)
    return jax.shard_map(layer_local, mesh=mesh,
                         in_specs=(row_spec, P('dp'), cache_spec, cache_spec, P(), col_spec, col_spec,
                                   col_spec, split_rows, P(), col_spec, col_spec, split_rows),
                         out_specs=(row_spec, cache_spec, cache_spec), check_vma=False)
```

```python
import functools
import math
import numpy as np
import jax
import jax.numpy as jnp
from jax import lax
from jax.experimental import pallas as pl
from jax.experimental.pallas import tpu as pltpu
from jax.sharding import PartitionSpec as P

EPS = 1e-5
ROPE_THETA = 500000.0
ROPE_FACTOR = 8.0
LOW_FACTOR = 1.0
HIGH_FACTOR = 4.0
ORIG_CTX = 8192.0
MESH = pl.DeviceIdType.MESH
F32 = jnp.float32
BF16 = jnp.bfloat16

HEAD = 64
PAIR = 128
GROUP = 4
SEQS = 16
SUB = 8
ROWS = 32
N_HALF = 2
W_PARTS = 2
SLOTS = 6
AHEAD = 3


def frequency_lanes():
    half = HEAD // 2
    exponents = np.arange(half, dtype=np.float32) * np.float32(2.0 / HEAD)
    inv_freq = (1.0 / np.power(np.float32(ROPE_THETA), exponents)).astype(np.float32)
    wavelen = (2.0 * math.pi) / inv_freq
    smooth = (ORIG_CTX / wavelen - LOW_FACTOR) / (HIGH_FACTOR - LOW_FACTOR)
    blended = (1.0 - smooth) * inv_freq / ROPE_FACTOR + smooth * inv_freq
    inv_freq = np.where(wavelen < ORIG_CTX / HIGH_FACTOR, inv_freq,
                        np.where(wavelen > ORIG_CTX / LOW_FACTOR, inv_freq / ROPE_FACTOR, blended))
    lanes = np.arange(PAIR)
    freq = inv_freq[lanes % half].astype(np.float32)
    sign = np.where(lanes % HEAD < half, -1.0, 1.0).astype(np.float32)
    return np.stack([freq, sign])


def layer_kernel(pos_hbm, freq_hbm, resid_hbm, gain_a_hbm, gain_m_hbm, wq_hbm, wk_hbm, wv_hbm, kc_hbm, vc_hbm,
                 wo_hbm, wg_hbm, wu_hbm, wd_hbm,
                 x1_hbm, send_hbm, knew_hbm, vnew_hbm,
                 pos_v, freq_v, resid_v, gain_a, gain_m, wq_v, wk_v, wv_v, k_buf, v_buf, wo_v, wg_v, wu_v, wd_v,
                 h_scr, a_scr, q_scr, k_scr, v_scr, pos_scr, s_scr, p_scr, n_scr,
                 part, near, mine, far, full, zsum,
                 in_sem, kv_sem, wo_sem, w_sem, out_sem,
                 near_send, near_recv, far_send, far_recv, back_send, back_recv):
    tp = lax.axis_index("tp")
    dp = lax.axis_index("dp")
    core = lax.rem(tp, 2)
    other = 1 - core
    sibling = tp + 1 - 2 * core
    partner = lax.rem(tp + 2, 4)
    n_seqs, dim = resid_v.shape
    cache_len = kc_hbm.shape[1]
    half_dim = dim // 2
    ffn = wg_v.shape[1]
    n_chunk = n_seqs // ROWS
    block = ROWS * PAIR

    inputs = [pltpu.make_async_copy(src, dst, in_sem.at[i]) for i, (src, dst) in enumerate((
        (resid_hbm, resid_v), (gain_a_hbm, gain_a), (wq_hbm, wq_v), (wk_hbm, wk_v), (wv_hbm, wv_v),
        (pos_hbm, pos_v), (freq_hbm, freq_v), (gain_m_hbm, gain_m)))]
    for c in inputs:
        c.start()

    def cache_copies(r, slot):
        at = pl.ds(pl.multiple_of(r * block, block), block)
        return (pltpu.make_async_copy(kc_hbm.at[at], k_buf.at[slot], kv_sem.at[0, slot]),
                pltpu.make_async_copy(vc_hbm.at[at], v_buf.at[slot], kv_sem.at[1, slot]))

    for c in cache_copies(0, 0):
        c.start()
    wo_copies = []
    for g in range(GROUP):
        for h in range(2):
            for s in range(2):
                wo_copies.append(pltpu.make_async_copy(
                    wo_hbm.at[pl.ds((h * GROUP + g) * HEAD, HEAD), pl.ds(s * half_dim, half_dim)],
                    wo_v.at[s, pl.ds((2 * g + h) * HEAD, HEAD), :], wo_sem.at[(2 * g + h) * 2 + s]))
    for c in wo_copies:
        c.start()
    for c in cache_copies(1, 1):
        c.start()
    w_copies = []
    for src, dst in ((wg_hbm, wg_v), (wu_hbm, wu_v), (wd_hbm, wd_v)):
        rows = dst.shape[0] // W_PARTS
        for i in range(W_PARTS):
            at = pl.ds(i * rows, rows)
            w_copies.append(pltpu.make_async_copy(src.at[at], dst.at[at], w_sem.at[len(w_copies)]))

    barrier = pltpu.get_barrier_semaphore()
    for peer in (sibling, partner):
        pl.semaphore_signal(barrier, inc=1, device_id=(dp, peer), device_id_type=MESH)

    def remote(src, dst, sems, k, r, peer):
        return pltpu.make_async_remote_copy(src_ref=src, dst_ref=dst, send_sem=sems[0].at[k, r], recv_sem=sems[1].at[k, r],
                                            device_id=(dp, peer), device_id_type=MESH)

    def chunk(r):
        return pl.ds(pl.multiple_of(r * ROWS, ROWS), ROWS)

    def near_copy(k, r):
        return remote(part.at[other, chunk(r)], near.at[chunk(r)], (near_send, near_recv), k, r, sibling)

    def far_copy(r):
        return remote(mine.at[chunk(r)], far.at[chunk(r)], (far_send, far_recv), 0, r, partner)

    def back_copy(r):
        return remote(full.at[core, chunk(r)], full.at[core, chunk(r)], (back_send, back_recv), 0, r, sibling)

    def sum_near(r):
        near_copy(0, r).wait_recv()
        mine[chunk(r), :] = part[core, chunk(r), :] + near[chunk(r), :]
        far_copy(r).start()

    my_cols = pl.ds(pl.multiple_of(core * half_dim, half_dim), half_dim)
    other_cols = pl.ds(pl.multiple_of(other * half_dim, half_dim), half_dim)

    for c in inputs[:2]:
        c.wait()
    gain_row = gain_a[...].astype(F32).reshape(1, dim)
    rows = 64
    for i in range(n_seqs // rows):
        x = resid_v[i * rows:(i + 1) * rows, :].astype(F32)
        mean_sq = jnp.sum(x * x, axis=1, keepdims=True) * (1.0 / dim)
        h_scr[i * rows:(i + 1) * rows, :] = (x * lax.rsqrt(mean_sq + EPS) * gain_row).astype(BF16)
    for c in inputs[2:]:
        c.wait()
    diag = (lax.broadcasted_iota(jnp.int32, (n_seqs, n_seqs), 0)
            == lax.broadcasted_iota(jnp.int32, (n_seqs, n_seqs), 1))
    pos_col = jnp.sum(jnp.where(diag, pos_v[...].astype(F32), 0.0), axis=1, keepdims=True)
    pos_scr[...] = jnp.broadcast_to(pos_col, (n_seqs, PAIR))
    angles = pos_scr[...] * freq_v[0:1, :]
    cos_t = jnp.cos(angles)
    sin_t = jnp.sin(angles) * freq_v[1:2, :]
    lane = lax.broadcasted_iota(jnp.int32, (n_seqs, PAIR), 1)
    low = lane % HEAD < HEAD // 2
    first = lane < HEAD

    def rope(t):
        t = t.astype(BF16).astype(F32)
        swapped = jnp.where(low, pltpu.roll(t, PAIR - HEAD // 2, 1), pltpu.roll(t, HEAD // 2, 1))
        return (t * cos_t + swapped * sin_t).astype(BF16).astype(F32)

    h = h_scr[...]
    tiles = [rope(jnp.dot(h, wq_v[:, t * PAIR:(t + 1) * PAIR], preferred_element_type=F32)) for t in range(GROUP)]
    for g in range(GROUP):
        lower, upper = tiles[g // 2], tiles[2 + g // 2]
        if g % 2 == 0:
            upper = pltpu.roll(upper, HEAD, 1)
        else:
            lower = pltpu.roll(lower, HEAD, 1)
        q_scr[g, :, :] = jnp.where(first, lower, upper)
    k_scr[...] = rope(jnp.dot(h, wk_v[...], preferred_element_type=F32))
    v_scr[...] = jnp.dot(h, wv_v[...], preferred_element_type=F32).astype(BF16).astype(F32)
    new_copies = (pltpu.make_async_copy(k_scr, knew_hbm, out_sem.at[0]), pltpu.make_async_copy(v_scr, vnew_hbm, out_sem.at[1]))
    for c in new_copies:
        c.start()
    for c in wo_copies:
        c.wait()
    pl.semaphore_wait(barrier, 2)

    lane_q = lax.broadcasted_iota(jnp.int32, (SUB, PAIR), 1)
    sub_q = lax.broadcasted_iota(jnp.int32, (SUB, PAIR), 0)
    head_mask = [lane_q < HEAD, lane_q >= HEAD]
    lane_p = lax.broadcasted_iota(jnp.int32, (SUB, cache_len), 1).astype(F32)
    stack = lambda x: jnp.concatenate([x] * (2 * GROUP), axis=0)

    tall = 2 * GROUP * SUB

    def attend(r, slot):
        scale = 1.0 / math.sqrt(HEAD)
        tiles_at = [pl.multiple_of(r * ROWS + t * SUB, SUB) for t in range(ROWS // SUB)]
        for t, base in enumerate(tiles_at):
            q_rows = []
            for g in range(GROUP):
                q_g = q_scr[g, pl.ds(base, SUB), :]
                for hd in range(2):
                    q_rows.append(jnp.where(head_mask[hd], q_g, 0.0))
            q_bd = jnp.concatenate([jnp.concatenate([jnp.where(sub_q == b, q, 0.0) for b in range(SUB)], axis=1)
                                    for q in q_rows], axis=0).astype(BF16)
            q_all = jnp.concatenate(q_rows, axis=0)
            at = slice(t * tall, (t + 1) * tall)
            n_scr[at, :] = jnp.broadcast_to(
                jnp.sum(q_all * stack(k_scr[pl.ds(base, SUB), :]), axis=1, keepdims=True) * scale, (tall, PAIR))
            s_scr[at, :] = jnp.dot(q_bd, k_buf[slot, t * SUB * PAIR:(t + 1) * SUB * PAIR, :],
                                   preferred_element_type=F32) * scale
        for t, base in enumerate(tiles_at):
            at = slice(t * tall, (t + 1) * tall)
            old = stack(lane_p < pos_scr[pl.ds(base, SUB), 0:1])
            scores = jnp.where(old, s_scr[at, :], -jnp.inf)
            score_new = n_scr[at, 0:1]
            top = jnp.maximum(jnp.max(scores, axis=1, keepdims=True), score_new)
            expd = jnp.exp(scores - top)
            exp_new = jnp.exp(score_new - top)
            inv = 1.0 / (jnp.sum(expd, axis=1, keepdims=True) + exp_new)
            p_scr[at, :] = (expd * inv).astype(BF16)
            n_scr[at, :] = jnp.broadcast_to((exp_new * inv).astype(BF16).astype(F32), (tall, PAIR))
        outs = []
        for t, base in enumerate(tiles_at):
            v_new = v_scr[pl.ds(base, SUB), :]
            mixed = lax.dot_general(p_scr[t * tall:(t + 1) * tall, :], v_buf[slot, t * SUB * PAIR:(t + 1) * SUB * PAIR, :],
                                    (((1,), (1,)), ((), ())), preferred_element_type=F32)
            pieces = []
            for g in range(GROUP):
                acc = None
                for hd in range(2):
                    lo = (g * 2 + hd) * SUB
                    piece = mixed[lo:lo + SUB, 0:PAIR]
                    for b in range(1, SUB):
                        piece = jnp.where(sub_q == b, mixed[lo:lo + SUB, b * PAIR:(b + 1) * PAIR], piece)
                    piece = piece + n_scr[t * tall + lo:t * tall + lo + SUB, :] * v_new
                    acc = piece if acc is None else jnp.where(head_mask[1], piece, acc)
                pieces.append(acc)
            outs.append(jnp.concatenate(pieces, axis=1))
        return jnp.concatenate(outs, axis=0).astype(BF16)

    def chunk_step(r, carry):
        slot = lax.rem(r, 2)
        for c in cache_copies(r, slot):
            c.wait()
        o = attend(r, slot)

        @pl.when(r + 2 < n_chunk)
        def _next():
            for c in cache_copies(r + 2, slot):
                c.start()

        for i, c in enumerate(w_copies):
            pl.when(r == i + 1)(c.start)

        part[other, chunk(r), :] = jnp.dot(o, wo_v[other], preferred_element_type=F32)
        near_copy(0, r).start()
        part[core, chunk(r), :] = jnp.dot(o, wo_v[core], preferred_element_type=F32)

        @pl.when(r > 0)
        def _sum():
            sum_near(r - 1)
        return carry

    lax.fori_loop(0, n_chunk, chunk_step, 0)
    sum_near(n_chunk - 1)
    for r in range(n_chunk):
        near_copy(0, r).wait_send()

    def sum_far_y(r):
        far_copy(r).wait_recv()
        total = resid_v[chunk(r), my_cols].astype(F32) + (mine[chunk(r), :] + far[chunk(r), :])
        full[core, chunk(r), :] = total.astype(BF16).astype(F32)
        back_copy(r).start()

    sends = []
    gain_row2 = gain_m[...].astype(F32).reshape(1, dim)
    tile = 512
    per_half = n_chunk // N_HALF
    half_rows = n_seqs // N_HALF
    for m in range(N_HALF):
        chunks = range(m * per_half, (m + 1) * per_half)
        def normalize(r):
            back_copy(r).wait_recv()
            x0 = full[0, chunk(r), :]
            x1 = full[1, chunk(r), :]
            mean_sq = (jnp.sum(x0 * x0, axis=1, keepdims=True)
                       + jnp.sum(x1 * x1, axis=1, keepdims=True)) * (1.0 / dim)
            inv = lax.rsqrt(mean_sq + EPS)
            at = pl.ds((r - chunks[0]) * ROWS, ROWS)
            h_scr[at, :half_dim] = (x0 * inv * gain_row2[:, :half_dim]).astype(BF16)
            h_scr[at, half_dim:] = (x1 * inv * gain_row2[:, half_dim:]).astype(BF16)

        for r in chunks:
            sum_far_y(r)
            if r > chunks[0]:
                normalize(r - 1)
        normalize(chunks[-1])
        if m == 0:
            for c in w_copies[:2 * W_PARTS]:
                c.wait()

        def up_tile(n, carry):
            cols = pl.ds(pl.multiple_of(n * tile, tile), tile)
            h2 = h_scr[0:half_rows, :]
            gate = jnp.dot(h2, wg_v[:, cols], preferred_element_type=F32).astype(BF16).astype(F32)
            up = jnp.dot(h2, wu_v[:, cols], preferred_element_type=F32).astype(BF16).astype(F32)
            a_scr[:, cols] = (gate * jax.nn.sigmoid(gate) * up).astype(BF16)
            return carry

        lax.fori_loop(0, ffn // tile, up_tile, 0)
        if m == 0:
            for c in w_copies[2 * W_PARTS:]:
                c.wait()
        half_at = pl.ds(m * half_rows, half_rows)
        for s in (other, core):
            def down_tile(n, carry, s=s):
                cols = pl.ds(pl.multiple_of(s * half_dim + n * tile, tile), tile)
                part[s, half_at, pl.ds(pl.multiple_of(n * tile, tile), tile)] = jnp.dot(
                    a_scr[...], wd_v[:, cols], preferred_element_type=F32)
                return carry

            lax.fori_loop(0, half_dim // tile, down_tile, 0)
            if s is other:
                for r in chunks:
                    near_copy(1, r).start()
        for r in chunks:
            near_copy(1, r).wait_recv()
            zsum[chunk(r), :] = part[core, chunk(r), :] + near[chunk(r), :]
        sends += [pltpu.make_async_copy(full.at[core, half_at], x1_hbm.at[half_at], out_sem.at[4 + m]),
                  pltpu.make_async_copy(zsum.at[half_at], send_hbm.at[half_at], out_sem.at[2 + m])]
        for c in sends[-2:]:
            c.start()

    for c in (*new_copies, *sends):
        c.wait()
    for r in range(n_chunk):
        near_copy(1, r).wait_send()
        back_copy(r).wait_send()
        far_copy(r).wait_send()


def layer_call(resid_in, positions, kc, vc, gain_attn, w_query, w_key, w_value, w_out, gain_mlp, w_gate, w_up, w_down):
    n_seqs, dim = resid_in.shape
    half = dim // 2
    ffn = w_gate.shape[1]
    cache_len = kc.shape[1]
    n_chunk = n_seqs // ROWS
    hbm = pl.BlockSpec(memory_space=pl.ANY)
    sems = pltpu.SemaphoreType.DMA((2, n_chunk))
    freq = jnp.asarray(frequency_lanes())
    args = (positions.reshape(1, n_seqs), freq, resid_in, gain_attn, gain_mlp,
            w_query, w_key, w_value, kc, vc, w_out, w_gate, w_up, w_down)
    return pl.pallas_call(
        layer_kernel,
        out_shape=(jax.ShapeDtypeStruct((n_seqs, half), F32), jax.ShapeDtypeStruct((n_seqs, half), F32),
                   jax.ShapeDtypeStruct((n_seqs, PAIR), F32), jax.ShapeDtypeStruct((n_seqs, PAIR), F32)),
        in_specs=[hbm] * len(args),
        out_specs=(hbm,) * 4,
        scratch_shapes=[
            pltpu.VMEM((1, n_seqs), jnp.int32), pltpu.VMEM(freq.shape, F32), pltpu.VMEM((n_seqs, dim), BF16),
            pltpu.VMEM((dim,), BF16), pltpu.VMEM((dim,), BF16),
            pltpu.VMEM(w_query.shape, BF16), pltpu.VMEM(w_key.shape, BF16), pltpu.VMEM(w_value.shape, BF16),
            pltpu.VMEM((2, ROWS * PAIR, cache_len), BF16), pltpu.VMEM((2, ROWS * PAIR, cache_len), BF16),
            pltpu.VMEM((2, w_out.shape[0], half), BF16), pltpu.VMEM(w_gate.shape, BF16),
            pltpu.VMEM(w_up.shape, BF16), pltpu.VMEM(w_down.shape, BF16),
            pltpu.VMEM((n_seqs, dim), BF16), pltpu.VMEM((n_seqs // N_HALF, ffn), BF16),
            pltpu.VMEM((GROUP, n_seqs, PAIR), F32), pltpu.VMEM((n_seqs, PAIR), F32),
            pltpu.VMEM((n_seqs, PAIR), F32), pltpu.VMEM((n_seqs, PAIR), F32),
            pltpu.VMEM((2 * GROUP * ROWS, cache_len), F32), pltpu.VMEM((2 * GROUP * ROWS, cache_len), BF16),
            pltpu.VMEM((2 * GROUP * ROWS, PAIR), F32),
            pltpu.VMEM((2, n_seqs, half), F32), pltpu.VMEM((n_seqs, half), F32),
            pltpu.VMEM((n_seqs, half), F32), pltpu.VMEM((n_seqs, half), F32),
            pltpu.VMEM((2, n_seqs, half), F32), pltpu.VMEM((n_seqs, half), F32),
            pltpu.SemaphoreType.DMA((8,)), pltpu.SemaphoreType.DMA((2, 2)), pltpu.SemaphoreType.DMA((16,)),
            pltpu.SemaphoreType.DMA((3 * W_PARTS,)), pltpu.SemaphoreType.DMA((6,)),
            sems, sems, sems, sems, sems, sems],
        compiler_params=pltpu.CompilerParams(collective_id=0, has_side_effects=True, vmem_limit_bytes=67043328),
        name="layer",
    )(*args)


def write_kernel(first_step, n_steps, pos_smem, knew_hbm, vnew_hbm, kc_hbm, vc_hbm, *refs):
    ko_hbm, vo_hbm, k_buf, v_buf, knew, vnew, new_sem, in_sem, out_sem = refs[-9:]
    cache_len = kc_hbm.shape[1]
    block = SEQS * PAIR
    width = PAIR
    lane = lax.broadcasted_iota(jnp.int32, (PAIR, width), 1)

    def copies(step):
        slot = lax.rem(step, SLOTS)
        at = pl.ds(pl.multiple_of((first_step + step) * block, block), block)
        return ((pltpu.make_async_copy(kc_hbm.at[at], k_buf.at[slot], in_sem.at[0, slot]),
                 pltpu.make_async_copy(vc_hbm.at[at], v_buf.at[slot], in_sem.at[1, slot])),
                (pltpu.make_async_copy(k_buf.at[slot], ko_hbm.at[at], out_sem.at[0, slot]),
                 pltpu.make_async_copy(v_buf.at[slot], vo_hbm.at[at], out_sem.at[1, slot])))

    for step in range(min(AHEAD, n_steps)):
        for c in copies(step)[0]:
            c.start()
    news = (pltpu.make_async_copy(knew_hbm, knew, new_sem.at[0]), pltpu.make_async_copy(vnew_hbm, vnew, new_sem.at[1]))
    for c in news:
        c.start()
    for c in news:
        c.wait()

    def body(step, carry):
        slot = lax.rem(step, SLOTS)
        ins, outs = copies(step)
        for c in ins:
            c.wait()

        @pl.when(step + AHEAD < n_steps)
        def _next():
            @pl.when(step + AHEAD >= SLOTS)
            def _free():
                for c in copies(step + AHEAD - SLOTS)[1]:
                    c.wait()
            for c in copies(step + AHEAD)[0]:
                c.start()

        for t in range(SEQS // SUB):
            base = pl.multiple_of((first_step + step) * SEQS + t * SUB, SUB)
            k_t = knew[pl.ds(base, SUB), :].T
            v_t = vnew[pl.ds(base, SUB), :].T
            for b in range(SUB):
                pos = pos_smem[base + b]
                lo = pl.multiple_of(pos // width * width, width)
                hit = lane == pos - lo
                at = pl.ds((t * SUB + b) * PAIR, PAIR)
                cols = pl.ds(lo, width)
                k_buf[slot, at, cols] = jnp.where(hit, k_t[:, b:b + 1], k_buf[slot, at, cols].astype(F32)).astype(BF16)
                v_buf[slot, at, cols] = jnp.where(hit, v_t[:, b:b + 1], v_buf[slot, at, cols].astype(F32)).astype(BF16)
        for c in outs:
            c.start()
        return carry

    lax.fori_loop(0, n_steps, body, 0)
    for step in range(max(0, n_steps - SLOTS), n_steps):
        for c in copies(step)[1]:
            c.wait()


def write_call(positions, knew, vnew, kc, vc, first_step, n_steps, prev=()):
    cache_len = kc.shape[1]
    hbm = pl.BlockSpec(memory_space=pl.ANY)
    buf = pltpu.VMEM((SLOTS, SEQS * PAIR, cache_len), BF16)
    return pl.pallas_call(
        functools.partial(write_kernel, first_step, n_steps),
        out_shape=(jax.ShapeDtypeStruct(kc.shape, BF16), jax.ShapeDtypeStruct(vc.shape, BF16)),
        in_specs=[pl.BlockSpec(memory_space=pltpu.SMEM)] + [hbm] * (4 + len(prev)),
        out_specs=(hbm, hbm),
        scratch_shapes=[buf, buf, pltpu.VMEM(knew.shape, F32), pltpu.VMEM(vnew.shape, F32), pltpu.SemaphoreType.DMA((2,)),
                        pltpu.SemaphoreType.DMA((2, SLOTS)), pltpu.SemaphoreType.DMA((2, SLOTS))],
        input_output_aliases={5 + i: i for i in range(len(prev))},
        compiler_params=pltpu.CompilerParams(vmem_limit_bytes=60 << 20),
        cost_estimate=pl.CostEstimate(flops=10 ** 10, bytes_accessed=4 * SEQS * PAIR * cache_len * 2 * n_steps,
                                      transcendentals=0),
        name="write",
    )(positions, knew, vnew, kc, vc, *prev)


def join_kernel(core_smem, mine_ref, other_ref, out_ref):
    half = mine_ref.shape[1]
    low = core_smem[0] == 0
    mine, other = mine_ref[...], other_ref[...]
    out_ref[:, :half] = jnp.where(low, mine, other).astype(BF16)
    out_ref[:, half:] = jnp.where(low, other, mine).astype(BF16)


def join_call(mine, other):
    n_seqs, half = mine.shape
    rows = 128
    one = pl.BlockSpec((rows, half), lambda i, c: (i, 0))
    return pl.pallas_call(
        join_kernel,
        out_shape=jax.ShapeDtypeStruct((n_seqs, 2 * half), BF16),
        grid_spec=pltpu.PrefetchScalarGridSpec(
            num_scalar_prefetch=1, grid=(n_seqs // rows,), in_specs=[one, one],
            out_specs=pl.BlockSpec((rows, 2 * half), lambda i, c: (i, 0))),
        compiler_params=pltpu.CompilerParams(dimension_semantics=("arbitrary",), vmem_limit_bytes=8 << 20),
        name="join",
    )((lax.axis_index('tp') % 2).reshape(1), mine, other)


FAR = [(0, 2), (1, 3), (2, 0), (3, 1)]
NEAR = [(0, 1), (1, 0), (2, 3), (3, 2)]


def solution(mesh):
    def layer_local(resid_in, positions, k_cache, v_cache, gain_attn, w_query, w_key, w_value,
                    w_out, gain_mlp, w_gate, w_up, w_down):
        n_seqs, cache_len, heads, dim = k_cache.shape
        flat = lambda c: jnp.transpose(c, (0, 2, 3, 1)).reshape(n_seqs * heads * dim, cache_len)
        back = lambda c: jnp.transpose(c.reshape(n_seqs, heads, dim, cache_len), (0, 3, 1, 2))
        kc, vc = flat(k_cache), flat(v_cache)
        x1, send, knew, vnew = layer_call(resid_in, positions, kc, vc, gain_attn, w_query, w_key, w_value,
                                                     w_out, gain_mlp, w_gate, w_up, w_down)
        far = lax.ppermute(send, 'tp', FAR)
        k_full, v_full = write_call(positions, knew, vnew, kc, vc, 0, n_seqs // SEQS)
        far, k_full, v_full = lax.optimization_barrier((far, k_full, v_full))
        total = x1 + (send + far)
        total_other = lax.ppermute(total, 'tp', NEAR)
        resid_out = join_call(total, total_other)
        return resid_out, back(k_full), back(v_full)

    row_spec = P('dp', None)
    cache_spec = P('dp', None, 'tp', None)
    col_spec = P(None, 'tp')
    split_rows = P('tp', None)
    return jax.shard_map(layer_local, mesh=mesh,
                         in_specs=(row_spec, P('dp'), cache_spec, cache_spec, P(), col_spec, col_spec,
                                   col_spec, split_rows, P(), col_spec, col_spec, split_rows),
                         out_specs=(row_spec, cache_spec, cache_spec), check_vma=False)
```

```python
import functools
import math
import numpy as np
import jax
import jax.numpy as jnp
from jax import lax
from jax.experimental import pallas as pl
from jax.experimental.pallas import tpu as pltpu
from jax.sharding import PartitionSpec as P

EPS = 1e-5
ROPE_THETA = 500000.0
ROPE_FACTOR = 8.0
LOW_FACTOR = 1.0
HIGH_FACTOR = 4.0
ORIG_CTX = 8192.0
MESH = pl.DeviceIdType.MESH
F32 = jnp.float32
BF16 = jnp.bfloat16

HEAD = 64
PAIR = 128
GROUP = 4
SEQS = 16
SUB = 8
ROWS = 32
BLOCK = 32
FIRST = 64
PARTS = ((0, 4), (4, 8))
LAYER_VMEM = 67043328
W_PARTS = 4
SLOTS = 16
AHEAD = 16


def frequency_lanes():
    half = HEAD // 2
    exponents = np.arange(half, dtype=np.float32) * np.float32(2.0 / HEAD)
    inv_freq = (1.0 / np.power(np.float32(ROPE_THETA), exponents)).astype(np.float32)
    wavelen = (2.0 * math.pi) / inv_freq
    smooth = (ORIG_CTX / wavelen - LOW_FACTOR) / (HIGH_FACTOR - LOW_FACTOR)
    blended = (1.0 - smooth) * inv_freq / ROPE_FACTOR + smooth * inv_freq
    inv_freq = np.where(wavelen < ORIG_CTX / HIGH_FACTOR, inv_freq,
                        np.where(wavelen > ORIG_CTX / LOW_FACTOR, inv_freq / ROPE_FACTOR, blended))
    lanes = np.arange(PAIR)
    freq = inv_freq[lanes % half].astype(np.float32)
    sign = np.where(lanes % HEAD < half, -1.0, 1.0).astype(np.float32)
    return np.stack([freq, sign])


def layer_kernel(pos_hbm, freq_hbm, resid_hbm, gain_a_hbm, gain_m_hbm, wq_hbm, wk_hbm, wv_hbm, kc_hbm, vc_hbm,
                 wo_hbm, wg_hbm, wu_hbm, wd_hbm,
                 x1_hbm, send_hbm, knew_hbm, vnew_hbm,
                 pos_v, freq_v, resid_v, gain_a, gain_m, wq_v, wk_v, wv_v, k_buf, v_buf, wo_v, wg_v, wu_v, wd_v,
                 h_scr, a_scr, q_scr, k_scr, v_scr, pos_scr, s_scr, p_scr, n_scr,
                 part, near, mine, far, full, zsum,
                 in_sem, kv_sem, wo_sem, w_sem, out_sem,
                 near_send, near_recv, far_send, far_recv, back_send, back_recv):
    tp = lax.axis_index("tp")
    dp = lax.axis_index("dp")
    core = lax.rem(tp, 2)
    other = 1 - core
    sibling = tp + 1 - 2 * core
    partner = lax.rem(tp + 2, 4)
    n_seqs, dim = resid_v.shape
    cache_len = kc_hbm.shape[1]
    half_dim = dim // 2
    ffn = wg_v.shape[1]
    n_chunk = n_seqs // ROWS
    block = BLOCK * PAIR

    inputs = [pltpu.make_async_copy(src, dst, in_sem.at[i]) for i, (src, dst) in enumerate((
        (resid_hbm, resid_v), (gain_a_hbm, gain_a), (wq_hbm, wq_v), (wk_hbm, wk_v), (wv_hbm, wv_v),
        (pos_hbm, pos_v), (freq_hbm, freq_v), (gain_m_hbm, gain_m)))]
    for c in inputs:
        c.start()

    def cache_copies(r, slot):
        at = pl.ds(pl.multiple_of(r * block, block), block)
        return (pltpu.make_async_copy(kc_hbm.at[at], k_buf.at[slot], kv_sem.at[0, slot]),
                pltpu.make_async_copy(vc_hbm.at[at], v_buf.at[slot], kv_sem.at[1, slot]))

    wo_copies = []
    for g in range(GROUP):
        for h in range(2):
            for s in range(2):
                wo_copies.append(pltpu.make_async_copy(
                    wo_hbm.at[pl.ds((h * GROUP + g) * HEAD, HEAD), pl.ds(s * half_dim, half_dim)],
                    wo_v.at[s, pl.ds((2 * g + h) * HEAD, HEAD), :], wo_sem.at[(2 * g + h) * 2 + s]))
    w_copies = []
    for src, dst in ((wg_hbm, wg_v), (wu_hbm, wu_v), (wd_hbm, wd_v)):
        rows = dst.shape[0] // W_PARTS
        for i in range(W_PARTS):
            at = pl.ds(i * rows, rows)
            w_copies.append(pltpu.make_async_copy(src.at[at], dst.at[at], w_sem.at[len(w_copies)]))

    barrier = pltpu.get_barrier_semaphore()
    for peer in (sibling, partner):
        pl.semaphore_signal(barrier, inc=1, device_id=(dp, peer), device_id_type=MESH)

    def remote(src, dst, sems, k, r, peer):
        return pltpu.make_async_remote_copy(src_ref=src, dst_ref=dst, send_sem=sems[0].at[k, r], recv_sem=sems[1].at[k, r],
                                            device_id=(dp, peer), device_id_type=MESH)

    def chunk(r):
        return pl.ds(pl.multiple_of(r * ROWS, ROWS), ROWS)

    def near_copy(k, r):
        return remote(part.at[other, chunk(r)], near.at[chunk(r)], (near_send, near_recv), k, r, sibling)

    def far_copy(r):
        return remote(mine.at[chunk(r)], far.at[chunk(r)], (far_send, far_recv), 0, r, partner)

    def back_copy(r):
        return remote(full.at[core, chunk(r)], full.at[core, chunk(r)], (back_send, back_recv), 0, r, sibling)

    def sum_near(r):
        near_copy(0, r).wait_recv()
        mine[chunk(r), :] = part[core, chunk(r), :] + near[chunk(r), :]
        far_copy(r).start()

    my_cols = pl.ds(pl.multiple_of(core * half_dim, half_dim), half_dim)
    other_cols = pl.ds(pl.multiple_of(other * half_dim, half_dim), half_dim)

    for c in inputs[:2]:
        c.wait()
    for c in cache_copies(0, 0):
        c.start()
    gain_row = gain_a[...].astype(F32).reshape(1, dim)

    def normalize_in(lo, hi):
        for i in range(lo, hi, FIRST):
            x = resid_v[i:i + FIRST, :].astype(F32)
            mean_sq = jnp.sum(x * x, axis=1, keepdims=True) * (1.0 / dim)
            h_scr[i:i + FIRST, :] = (x * lax.rsqrt(mean_sq + EPS) * gain_row).astype(BF16)

    def project(lo, hi):
        n = hi - lo
        at = slice(lo, hi)
        angles = pos_scr[at, :] * freq_v[0:1, :]
        cos_t = jnp.cos(angles)
        sin_t = jnp.sin(angles) * freq_v[1:2, :]
        lane = lax.broadcasted_iota(jnp.int32, (n, PAIR), 1)
        low = lane % HEAD < HEAD // 2
        first = lane < HEAD

        def rope(t):
            t = t.astype(BF16).astype(F32)
            swapped = jnp.where(low, pltpu.roll(t, PAIR - HEAD // 2, 1), pltpu.roll(t, HEAD // 2, 1))
            return (t * cos_t + swapped * sin_t).astype(BF16).astype(F32)

        h = h_scr[at, :]
        q_all = jnp.dot(h, wq_v[...], preferred_element_type=F32)
        tiles = [rope(q_all[:, t * PAIR:(t + 1) * PAIR]) for t in range(GROUP)]
        for g in range(GROUP):
            lower, upper = tiles[g // 2], tiles[2 + g // 2]
            if g % 2 == 0:
                upper = pltpu.roll(upper, HEAD, 1)
            else:
                lower = pltpu.roll(lower, HEAD, 1)
            q_scr[g, at, :] = jnp.where(first, lower, upper)
        k_scr[at, :] = rope(jnp.dot(h, wk_v[...], preferred_element_type=F32))
        v_scr[at, :] = jnp.dot(h, wv_v[...], preferred_element_type=F32).astype(BF16).astype(F32)

    normalize_in(0, FIRST)
    for c in inputs[2:]:
        c.wait()
    for c in (*wo_copies, *cache_copies(1, 1)):
        c.start()
    diag = (lax.broadcasted_iota(jnp.int32, (n_seqs, n_seqs), 0)
            == lax.broadcasted_iota(jnp.int32, (n_seqs, n_seqs), 1))
    pos_col = jnp.sum(jnp.where(diag, pos_v[...].astype(F32), 0.0), axis=1, keepdims=True)
    pos_scr[...] = jnp.broadcast_to(pos_col, (n_seqs, PAIR))
    project(0, FIRST)
    for c in wo_copies:
        c.wait()
    pl.semaphore_wait(barrier, 2)

    lane_q = lax.broadcasted_iota(jnp.int32, (SUB, PAIR), 1)
    sub_q = lax.broadcasted_iota(jnp.int32, (SUB, PAIR), 0)
    head_mask = [lane_q < HEAD, lane_q >= HEAD]
    lane_p = lax.broadcasted_iota(jnp.int32, (SUB, cache_len), 1).astype(F32)
    stack = lambda x: jnp.concatenate([x] * (2 * GROUP), axis=0)

    tall = 2 * GROUP * SUB

    def attend(first_row, slot):
        scale = 1.0 / math.sqrt(HEAD)
        tiles_at = [pl.multiple_of(first_row + t * SUB, SUB) for t in range(BLOCK // SUB)]
        for t, base in enumerate(tiles_at):
            q_rows = []
            for g in range(GROUP):
                q_g = q_scr[g, pl.ds(base, SUB), :]
                for hd in range(2):
                    q_rows.append(jnp.where(head_mask[hd], q_g, 0.0))
            q_bd = jnp.concatenate([jnp.concatenate([jnp.where(sub_q == b, q, 0.0) for b in range(SUB)], axis=1)
                                    for q in q_rows], axis=0).astype(BF16)
            q_all = jnp.concatenate(q_rows, axis=0)
            at = slice(t * tall, (t + 1) * tall)
            n_scr[at, :] = jnp.broadcast_to(
                jnp.sum(q_all * stack(k_scr[pl.ds(base, SUB), :]), axis=1, keepdims=True) * scale, (tall, PAIR))
            s_scr[at, :] = jnp.dot(q_bd, k_buf[slot, t * SUB * PAIR:(t + 1) * SUB * PAIR, :],
                                   preferred_element_type=F32) * scale
        for t, base in enumerate(tiles_at):
            at = slice(t * tall, (t + 1) * tall)
            old = stack(lane_p < pos_scr[pl.ds(base, SUB), 0:1])
            scores = jnp.where(old, s_scr[at, :], -jnp.inf)
            score_new = n_scr[at, 0:1]
            top = jnp.maximum(jnp.max(scores, axis=1, keepdims=True), score_new)
            expd = jnp.exp(scores - top)
            exp_new = jnp.exp(score_new - top)
            inv = 1.0 / (jnp.sum(expd, axis=1, keepdims=True) + exp_new)
            p_scr[at, :] = (expd * inv).astype(BF16)
            n_scr[at, :] = jnp.broadcast_to((exp_new * inv).astype(BF16).astype(F32), (tall, PAIR))
        outs = []
        for t, base in enumerate(tiles_at):
            v_new = v_scr[pl.ds(base, SUB), :]
            mixed = lax.dot_general(p_scr[t * tall:(t + 1) * tall, :], v_buf[slot, t * SUB * PAIR:(t + 1) * SUB * PAIR, :],
                                    (((1,), (1,)), ((), ())), preferred_element_type=F32)
            pieces = []
            for g in range(GROUP):
                acc = None
                for hd in range(2):
                    lo = (g * 2 + hd) * SUB
                    piece = mixed[lo:lo + SUB, 0:PAIR]
                    for b in range(1, SUB):
                        piece = jnp.where(sub_q == b, mixed[lo:lo + SUB, b * PAIR:(b + 1) * PAIR], piece)
                    piece = piece + n_scr[t * tall + lo:t * tall + lo + SUB, :] * v_new
                    acc = piece if acc is None else jnp.where(head_mask[1], piece, acc)
                pieces.append(acc)
            outs.append(jnp.concatenate(pieces, axis=1))
        return jnp.concatenate(outs, axis=0).astype(BF16)

    def pair_step(p, carry):
        for slot in range(2):
            r = 2 * p + slot
            for c in cache_copies(r, slot):
                c.wait()
            o = attend(r * ROWS, slot)

            @pl.when(r + 2 < n_chunk)
            def _next(r=r, slot=slot):
                for c in cache_copies(r + 2, slot):
                    c.start()

            for i, c in enumerate(w_copies):
                if (2 * i // 3) % 2 == slot:
                    pl.when(r == 2 * i // 3)(c.start)

            @pl.when(r > 1)
            def _sum(r=r):
                sum_near(r - 1)

            part[other, chunk(r), :] = jnp.dot(o, wo_v[other], preferred_element_type=F32)
            near_copy(0, r).start()
            part[core, chunk(r), :] = jnp.dot(o, wo_v[core], preferred_element_type=F32)

            if slot == 0:
                @pl.when(r == 0)
                def _others():
                    normalize_in(FIRST, n_seqs)
                    project(FIRST, n_seqs)
                    sum_near(0)
        return carry

    lax.fori_loop(0, n_chunk // 2, pair_step, 0)
    sum_near(n_chunk - 1)
    for r in range(n_chunk):
        near_copy(0, r).wait_send()

    def sum_far_y(r):
        far_copy(r).wait_recv()
        total = resid_v[chunk(r), my_cols].astype(F32) + (mine[chunk(r), :] + far[chunk(r), :])
        full[core, chunk(r), :] = total.astype(BF16).astype(F32)
        back_copy(r).start()

    gain_row2 = gain_m[...].astype(F32).reshape(1, dim)
    tile = 512
    outputs = [pltpu.make_async_copy(k_scr, knew_hbm, out_sem.at[2 * len(PARTS)]),
               pltpu.make_async_copy(v_scr, vnew_hbm, out_sem.at[2 * len(PARTS) + 1])]
    for c in outputs:
        c.start()
    for r in range(*PARTS[0]):
        sum_far_y(r)
    for m, (lo_chunk, hi_chunk) in enumerate(PARTS):
        chunks = range(lo_chunk, hi_chunk)
        n_rows = len(chunks) * ROWS

        def normalize(r):
            back_copy(r).wait_recv()
            x0 = full[0, chunk(r), :]
            x1 = full[1, chunk(r), :]
            mean_sq = (jnp.sum(x0 * x0, axis=1, keepdims=True)
                       + jnp.sum(x1 * x1, axis=1, keepdims=True)) * (1.0 / dim)
            inv = lax.rsqrt(mean_sq + EPS)
            at = pl.ds((r - chunks[0]) * ROWS, ROWS)
            h_scr[at, :half_dim] = (x0 * inv * gain_row2[:, :half_dim]).astype(BF16)
            h_scr[at, half_dim:] = (x1 * inv * gain_row2[:, half_dim:]).astype(BF16)

        for r in chunks:
            normalize(r)
        if m == 0:
            for c in w_copies[:2 * W_PARTS]:
                c.wait()

        def up_tile(n, carry, n_rows=n_rows):
            cols = pl.ds(pl.multiple_of(n * tile, tile), tile)
            h2 = h_scr[0:n_rows, :]
            gate = jnp.dot(h2, wg_v[:, cols], preferred_element_type=F32).astype(BF16).astype(F32)
            up = jnp.dot(h2, wu_v[:, cols], preferred_element_type=F32).astype(BF16).astype(F32)
            a_scr[0:n_rows, cols] = (gate * jax.nn.sigmoid(gate) * up).astype(BF16)
            return carry

        lax.fori_loop(0, ffn // tile, up_tile, 0)
        if m == 0:
            for c in w_copies[2 * W_PARTS:]:
                c.wait()
        part_at = pl.ds(lo_chunk * ROWS, n_rows)
        for s in (other, core):
            def down_tile(n, carry, s=s, part_at=part_at, n_rows=n_rows):
                cols = pl.ds(pl.multiple_of(s * half_dim + n * tile, tile), tile)
                part[s, part_at, pl.ds(pl.multiple_of(n * tile, tile), tile)] = jnp.dot(
                    a_scr[0:n_rows, :], wd_v[:, cols], preferred_element_type=F32)
                return carry

            lax.fori_loop(0, half_dim // tile, down_tile, 0)
            if s is other:
                for r in chunks:
                    near_copy(1, r).start()
        if m + 1 < len(PARTS):
            for r in range(*PARTS[m + 1]):
                sum_far_y(r)
        for r in chunks:
            near_copy(1, r).wait_recv()
            zsum[chunk(r), :] = part[core, chunk(r), :] + near[chunk(r), :]
        sends = (pltpu.make_async_copy(full.at[core, part_at], x1_hbm.at[part_at], out_sem.at[2 * m]),
                 pltpu.make_async_copy(zsum.at[part_at], send_hbm.at[part_at], out_sem.at[2 * m + 1]))
        for c in sends:
            c.start()
        outputs += sends

    for c in outputs:
        c.wait()
    for r in range(n_chunk):
        near_copy(1, r).wait_send()
        back_copy(r).wait_send()
        far_copy(r).wait_send()


def layer_call(resid_in, positions, kc, vc, gain_attn, w_query, w_key, w_value, w_out, gain_mlp, w_gate, w_up, w_down):
    n_seqs, dim = resid_in.shape
    half = dim // 2
    ffn = w_gate.shape[1]
    cache_len = kc.shape[1]
    n_chunk = n_seqs // ROWS
    hbm = pl.BlockSpec(memory_space=pl.ANY)
    sems = pltpu.SemaphoreType.DMA((2, n_chunk))
    freq = jnp.asarray(frequency_lanes())
    args = (positions.reshape(1, n_seqs), freq, resid_in, gain_attn, gain_mlp,
            w_query, w_key, w_value, kc, vc, w_out, w_gate, w_up, w_down)
    return pl.pallas_call(
        layer_kernel,
        out_shape=(jax.ShapeDtypeStruct((n_seqs, half), F32), jax.ShapeDtypeStruct((n_seqs, half), F32),
                   jax.ShapeDtypeStruct((n_seqs, PAIR), F32), jax.ShapeDtypeStruct((n_seqs, PAIR), F32)),
        in_specs=[hbm] * len(args),
        out_specs=(hbm,) * 4,
        scratch_shapes=[
            pltpu.VMEM((1, n_seqs), jnp.int32), pltpu.VMEM(freq.shape, F32), pltpu.VMEM((n_seqs, dim), BF16),
            pltpu.VMEM((dim,), BF16), pltpu.VMEM((dim,), BF16),
            pltpu.VMEM(w_query.shape, BF16), pltpu.VMEM(w_key.shape, BF16), pltpu.VMEM(w_value.shape, BF16),
            pltpu.VMEM((2, BLOCK * PAIR, cache_len), BF16), pltpu.VMEM((2, BLOCK * PAIR, cache_len), BF16),
            pltpu.VMEM((2, w_out.shape[0], half), BF16), pltpu.VMEM(w_gate.shape, BF16),
            pltpu.VMEM(w_up.shape, BF16), pltpu.VMEM(w_down.shape, BF16),
            pltpu.VMEM((n_seqs, dim), BF16), pltpu.VMEM((max(hi - lo for lo, hi in PARTS) * ROWS, ffn), BF16),
            pltpu.VMEM((GROUP, n_seqs, PAIR), F32), pltpu.VMEM((n_seqs, PAIR), F32),
            pltpu.VMEM((n_seqs, PAIR), F32), pltpu.VMEM((n_seqs, PAIR), F32),
            pltpu.VMEM((2 * GROUP * BLOCK, cache_len), F32), pltpu.VMEM((2 * GROUP * BLOCK, cache_len), BF16),
            pltpu.VMEM((2 * GROUP * BLOCK, PAIR), F32),
            pltpu.VMEM((2, n_seqs, half), F32), pltpu.VMEM((n_seqs, half), F32),
            pltpu.VMEM((n_seqs, half), F32), pltpu.VMEM((n_seqs, half), F32),
            pltpu.VMEM((2, n_seqs, half), F32), pltpu.VMEM((n_seqs, half), F32),
            pltpu.SemaphoreType.DMA((8,)), pltpu.SemaphoreType.DMA((2, 2)), pltpu.SemaphoreType.DMA((16,)),
            pltpu.SemaphoreType.DMA((3 * W_PARTS,)), pltpu.SemaphoreType.DMA((2 + 2 * len(PARTS),)),
            sems, sems, sems, sems, sems, sems],
        compiler_params=pltpu.CompilerParams(collective_id=0, has_side_effects=True, vmem_limit_bytes=LAYER_VMEM),
        name="layer",
    )(*args)


def write_kernel(first_step, n_steps, pos_smem, knew_hbm, vnew_hbm, kc_hbm, vc_hbm, *refs):
    ko_hbm, vo_hbm, k_buf, v_buf, knew, vnew, new_sem, in_sem, out_sem = refs[-9:]
    cache_len = kc_hbm.shape[1]
    block = SEQS * PAIR
    width = PAIR
    lane = lax.broadcasted_iota(jnp.int32, (PAIR, width), 1)

    def copies(step):
        slot = lax.rem(step, SLOTS)
        at = pl.ds(pl.multiple_of((first_step + step) * block, block), block)
        return ((pltpu.make_async_copy(kc_hbm.at[at], k_buf.at[slot], in_sem.at[0, slot]),
                 pltpu.make_async_copy(vc_hbm.at[at], v_buf.at[slot], in_sem.at[1, slot])),
                (pltpu.make_async_copy(k_buf.at[slot], ko_hbm.at[at], out_sem.at[0, slot]),
                 pltpu.make_async_copy(v_buf.at[slot], vo_hbm.at[at], out_sem.at[1, slot])))

    for step in range(min(AHEAD, n_steps)):
        for c in copies(step)[0]:
            c.start()
    news = (pltpu.make_async_copy(knew_hbm, knew, new_sem.at[0]), pltpu.make_async_copy(vnew_hbm, vnew, new_sem.at[1]))
    for c in news:
        c.start()
    for c in news:
        c.wait()

    def body(step, carry):
        slot = lax.rem(step, SLOTS)
        ins, outs = copies(step)
        for c in ins:
            c.wait()

        @pl.when(step + AHEAD < n_steps)
        def _next():
            @pl.when(step + AHEAD >= SLOTS)
            def _free():
                for c in copies(step + AHEAD - SLOTS)[1]:
                    c.wait()
            for c in copies(step + AHEAD)[0]:
                c.start()

        for t in range(SEQS // SUB):
            base = pl.multiple_of((first_step + step) * SEQS + t * SUB, SUB)
            k_t = knew[pl.ds(base, SUB), :].T
            v_t = vnew[pl.ds(base, SUB), :].T
            for b in range(SUB):
                pos = pos_smem[base + b]
                lo = pl.multiple_of(pos // width * width, width)
                hit = lane == pos - lo
                at = pl.ds((t * SUB + b) * PAIR, PAIR)
                cols = pl.ds(lo, width)
                k_buf[slot, at, cols] = jnp.where(hit, k_t[:, b:b + 1], k_buf[slot, at, cols].astype(F32)).astype(BF16)
                v_buf[slot, at, cols] = jnp.where(hit, v_t[:, b:b + 1], v_buf[slot, at, cols].astype(F32)).astype(BF16)
        for c in outs:
            c.start()
        return carry

    lax.fori_loop(0, n_steps, body, 0)
    for step in range(max(0, n_steps - SLOTS), n_steps):
        for c in copies(step)[1]:
            c.wait()


def write_call(positions, knew, vnew, kc, vc, first_step, n_steps, prev=()):
    cache_len = kc.shape[1]
    hbm = pl.BlockSpec(memory_space=pl.ANY)
    buf = pltpu.VMEM((SLOTS, SEQS * PAIR, cache_len), BF16)
    return pl.pallas_call(
        functools.partial(write_kernel, first_step, n_steps),
        out_shape=(jax.ShapeDtypeStruct(kc.shape, BF16), jax.ShapeDtypeStruct(vc.shape, BF16)),
        in_specs=[pl.BlockSpec(memory_space=pltpu.SMEM)] + [hbm] * (4 + len(prev)),
        out_specs=(hbm, hbm),
        scratch_shapes=[buf, buf, pltpu.VMEM(knew.shape, F32), pltpu.VMEM(vnew.shape, F32), pltpu.SemaphoreType.DMA((2,)),
                        pltpu.SemaphoreType.DMA((2, SLOTS)), pltpu.SemaphoreType.DMA((2, SLOTS))],
        input_output_aliases={5 + i: i for i in range(len(prev))},
        compiler_params=pltpu.CompilerParams(vmem_limit_bytes=60 << 20),
        cost_estimate=pl.CostEstimate(flops=10 ** 10, bytes_accessed=4 * SEQS * PAIR * cache_len * 2 * n_steps,
                                      transcendentals=0),
        name="write",
    )(positions, knew, vnew, kc, vc, *prev)


def join_kernel(core_smem, mine_ref, other_ref, out_ref):
    half = mine_ref.shape[1]
    low = core_smem[0] == 0
    mine, other = mine_ref[...], other_ref[...]
    out_ref[:, :half] = jnp.where(low, mine, other).astype(BF16)
    out_ref[:, half:] = jnp.where(low, other, mine).astype(BF16)


def join_call(mine, other):
    n_seqs, half = mine.shape
    rows = 128
    one = pl.BlockSpec((rows, half), lambda i, c: (i, 0))
    return pl.pallas_call(
        join_kernel,
        out_shape=jax.ShapeDtypeStruct((n_seqs, 2 * half), BF16),
        grid_spec=pltpu.PrefetchScalarGridSpec(
            num_scalar_prefetch=1, grid=(n_seqs // rows,), in_specs=[one, one],
            out_specs=pl.BlockSpec((rows, 2 * half), lambda i, c: (i, 0))),
        compiler_params=pltpu.CompilerParams(dimension_semantics=("arbitrary",), vmem_limit_bytes=8 << 20),
        name="join",
    )((lax.axis_index('tp') % 2).reshape(1), mine, other)


def total_kernel(x1_ref, send_ref, far_ref, out_ref):
    out_ref[...] = x1_ref[...] + (send_ref[...] + far_ref[...])


def total_call(x1, send, far):
    n_seqs, half = x1.shape
    rows = 128
    one = pl.BlockSpec((rows, half), lambda i: (i, 0))
    return pl.pallas_call(
        total_kernel,
        out_shape=jax.ShapeDtypeStruct(x1.shape, F32),
        grid=(n_seqs // rows,), in_specs=[one] * 3, out_specs=one,
        compiler_params=pltpu.CompilerParams(dimension_semantics=("arbitrary",), vmem_limit_bytes=16 << 20),
        name="total",
    )(x1, send, far)


FAR = [(0, 2), (1, 3), (2, 0), (3, 1)]
NEAR = [(0, 1), (1, 0), (2, 3), (3, 2)]


def solution(mesh):
    def layer_local(resid_in, positions, k_cache, v_cache, gain_attn, w_query, w_key, w_value,
                    w_out, gain_mlp, w_gate, w_up, w_down):
        n_seqs, cache_len, heads, dim = k_cache.shape
        flat = lambda c: jnp.transpose(c, (0, 2, 3, 1)).reshape(n_seqs * heads * dim, cache_len)
        back = lambda c: jnp.transpose(c.reshape(n_seqs, heads, dim, cache_len), (0, 3, 1, 2))
        kc, vc = flat(k_cache), flat(v_cache)
        x1, send, knew, vnew = layer_call(resid_in, positions, kc, vc, gain_attn, w_query, w_key, w_value,
                                                     w_out, gain_mlp, w_gate, w_up, w_down)
        far = lax.ppermute(send, 'tp', FAR)
        k_full, v_full = write_call(positions, knew, vnew, kc, vc, 0, n_seqs // SEQS)
        far, k_full, v_full = lax.optimization_barrier((far, k_full, v_full))
        total = total_call(x1, send, far)
        total_other = lax.ppermute(total, 'tp', NEAR)
        resid_out = join_call(total, total_other)
        return resid_out, back(k_full), back(v_full)

    row_spec = P('dp', None)
    cache_spec = P('dp', None, 'tp', None)
    col_spec = P(None, 'tp')
    split_rows = P('tp', None)
    return jax.shard_map(layer_local, mesh=mesh,
                         in_specs=(row_spec, P('dp'), cache_spec, cache_spec, P(), col_spec, col_spec,
                                   col_spec, split_rows, P(), col_spec, col_spec, split_rows),
                         out_specs=(row_spec, cache_spec, cache_spec), check_vma=False)
```

```python
import functools
import math
import numpy as np
import jax
import jax.numpy as jnp
from jax import lax
from jax.experimental import pallas as pl
from jax.experimental.pallas import tpu as pltpu
from jax.sharding import PartitionSpec as P

EPS = 1e-5
ROPE_THETA = 500000.0
ROPE_FACTOR = 8.0
LOW_FACTOR = 1.0
HIGH_FACTOR = 4.0
ORIG_CTX = 8192.0
MESH = pl.DeviceIdType.MESH
F32 = jnp.float32
BF16 = jnp.bfloat16

HEAD = 64
PAIR = 128
GROUP = 4
SEQS = 16
SUB = 8
ROWS = 32
BLOCK = 32
Z_IN = 1
FIRST = 64
PARTS = ((0, 4), (4, 8))
LAYER_VMEM = 67043328
WRITE_VMEM = 56 << 20
W_PARTS = 4
SLOTS = 16
AHEAD = 16


def frequency_lanes():
    half = HEAD // 2
    exponents = np.arange(half, dtype=np.float32) * np.float32(2.0 / HEAD)
    inv_freq = (1.0 / np.power(np.float32(ROPE_THETA), exponents)).astype(np.float32)
    wavelen = (2.0 * math.pi) / inv_freq
    smooth = (ORIG_CTX / wavelen - LOW_FACTOR) / (HIGH_FACTOR - LOW_FACTOR)
    blended = (1.0 - smooth) * inv_freq / ROPE_FACTOR + smooth * inv_freq
    inv_freq = np.where(wavelen < ORIG_CTX / HIGH_FACTOR, inv_freq,
                        np.where(wavelen > ORIG_CTX / LOW_FACTOR, inv_freq / ROPE_FACTOR, blended))
    lanes = np.arange(PAIR)
    freq = inv_freq[lanes % half].astype(np.float32)
    sign = np.where(lanes % HEAD < half, -1.0, 1.0).astype(np.float32)
    return np.stack([freq, sign])


def layer_kernel(pos_hbm, freq_hbm, resid_hbm, gain_a_hbm, gain_m_hbm, wq_hbm, wk_hbm, wv_hbm, kc_hbm, vc_hbm,
                 wo_hbm, wg_hbm, wu_hbm, wd_hbm,
                 x1_hbm, send_hbm, knew_hbm, vnew_hbm,
                 pos_v, freq_v, resid_v, gain_a, gain_m, wq_v, wk_v, wv_v, k_buf, v_buf, wo_v, wg_v, wu_v, wd_v,
                 h_scr, a_scr, q_scr, k_scr, v_scr, pos_scr, s_scr, p_scr, n_scr,
                 part, near, mine, far, full, zsum, zfar,
                 in_sem, kv_sem, wo_sem, w_sem, out_sem,
                 near_send, near_recv, far_send, far_recv, back_send, back_recv):
    tp = lax.axis_index("tp")
    dp = lax.axis_index("dp")
    core = lax.rem(tp, 2)
    other = 1 - core
    sibling = tp + 1 - 2 * core
    partner = lax.rem(tp + 2, 4)
    n_seqs, dim = resid_v.shape
    cache_len = kc_hbm.shape[1]
    half_dim = dim // 2
    ffn = wg_v.shape[1]
    n_chunk = n_seqs // ROWS
    block = BLOCK * PAIR
    tile = 512
    n_tile = half_dim // tile

    inputs = [pltpu.make_async_copy(src, dst, in_sem.at[i]) for i, (src, dst) in enumerate((
        (resid_hbm, resid_v), (gain_a_hbm, gain_a), (wq_hbm, wq_v), (wk_hbm, wk_v), (wv_hbm, wv_v),
        (pos_hbm, pos_v), (freq_hbm, freq_v), (gain_m_hbm, gain_m)))]
    for c in inputs:
        c.start()

    def cache_copies(r, slot):
        at = pl.ds(pl.multiple_of(r * block, block), block)
        return (pltpu.make_async_copy(kc_hbm.at[at], k_buf.at[slot], kv_sem.at[0, slot]),
                pltpu.make_async_copy(vc_hbm.at[at], v_buf.at[slot], kv_sem.at[1, slot]))

    wo_copies = []
    for g in range(GROUP):
        for h in range(2):
            for s in range(2):
                wo_copies.append(pltpu.make_async_copy(
                    wo_hbm.at[pl.ds((h * GROUP + g) * HEAD, HEAD), pl.ds(s * half_dim, half_dim)],
                    wo_v.at[s, pl.ds((2 * g + h) * HEAD, HEAD), :], wo_sem.at[(2 * g + h) * 2 + s]))
    w_copies = []
    for src, dst in ((wg_hbm, wg_v), (wu_hbm, wu_v), (wd_hbm, wd_v)):
        rows = dst.shape[0] // W_PARTS
        for i in range(W_PARTS):
            at = pl.ds(i * rows, rows)
            w_copies.append(pltpu.make_async_copy(src.at[at], dst.at[at], w_sem.at[len(w_copies)]))

    barrier = pltpu.get_barrier_semaphore()
    for peer in (sibling, partner):
        pl.semaphore_signal(barrier, inc=1, device_id=(dp, peer), device_id_type=MESH)

    def remote(src, dst, sems, k, r, peer):
        return pltpu.make_async_remote_copy(src_ref=src, dst_ref=dst, send_sem=sems[0].at[k, r], recv_sem=sems[1].at[k, r],
                                            device_id=(dp, peer), device_id_type=MESH)

    def chunk(r):
        return pl.ds(pl.multiple_of(r * ROWS, ROWS), ROWS)

    def near_copy(r):
        return remote(part.at[other, chunk(r)], near.at[chunk(r)], (near_send, near_recv), 0, r, sibling)

    def near_copy_z(m, at, n):
        cols = pl.ds(n * tile, tile)
        return remote(part.at[other, at, cols], near.at[at, cols], (near_send, near_recv), 1, m * n_tile + n, sibling)

    def far_copy(r):
        return remote(mine.at[chunk(r)], far.at[chunk(r)], (far_send, far_recv), 0, r, partner)

    def back_copy(r):
        return remote(full.at[core, chunk(r)], full.at[core, chunk(r)], (back_send, back_recv), 0, r, sibling)

    def far_copy_z(r):
        return remote(zsum.at[chunk(r)], zfar.at[chunk(r)], (far_send, far_recv), 1, r, partner)

    def sum_near(r):
        near_copy(r).wait_recv()
        mine[chunk(r), :] = part[core, chunk(r), :] + near[chunk(r), :]
        far_copy(r).start()

    my_cols = pl.ds(pl.multiple_of(core * half_dim, half_dim), half_dim)
    other_cols = pl.ds(pl.multiple_of(other * half_dim, half_dim), half_dim)

    for c in inputs[:2]:
        c.wait()
    for c in cache_copies(0, 0):
        c.start()
    gain_row = gain_a[...].astype(F32).reshape(1, dim)

    def normalize_in(lo, hi):
        for i in range(lo, hi, FIRST):
            x = resid_v[i:i + FIRST, :].astype(F32)
            mean_sq = jnp.sum(x * x, axis=1, keepdims=True) * (1.0 / dim)
            h_scr[i:i + FIRST, :] = (x * lax.rsqrt(mean_sq + EPS) * gain_row).astype(BF16)

    def project(lo, hi):
        n = hi - lo
        at = slice(lo, hi)
        angles = pos_scr[at, :] * freq_v[0:1, :]
        cos_t = jnp.cos(angles)
        sin_t = jnp.sin(angles) * freq_v[1:2, :]
        lane = lax.broadcasted_iota(jnp.int32, (n, PAIR), 1)
        low = lane % HEAD < HEAD // 2
        first = lane < HEAD

        def rope(t):
            t = t.astype(BF16).astype(F32)
            swapped = jnp.where(low, pltpu.roll(t, PAIR - HEAD // 2, 1), pltpu.roll(t, HEAD // 2, 1))
            return (t * cos_t + swapped * sin_t).astype(BF16).astype(F32)

        h = h_scr[at, :]
        q_all = jnp.dot(h, wq_v[...], preferred_element_type=F32)
        tiles = [rope(q_all[:, t * PAIR:(t + 1) * PAIR]) for t in range(GROUP)]
        for g in range(GROUP):
            lower, upper = tiles[g // 2], tiles[2 + g // 2]
            if g % 2 == 0:
                upper = pltpu.roll(upper, HEAD, 1)
            else:
                lower = pltpu.roll(lower, HEAD, 1)
            q_scr[g, at, :] = jnp.where(first, lower, upper)
        k_scr[at, :] = rope(jnp.dot(h, wk_v[...], preferred_element_type=F32))
        v_scr[at, :] = jnp.dot(h, wv_v[...], preferred_element_type=F32).astype(BF16).astype(F32)

    normalize_in(0, FIRST)
    for c in inputs[2:]:
        c.wait()
    for c in (*wo_copies, *cache_copies(1, 1)):
        c.start()
    diag = (lax.broadcasted_iota(jnp.int32, (n_seqs, n_seqs), 0)
            == lax.broadcasted_iota(jnp.int32, (n_seqs, n_seqs), 1))
    pos_col = jnp.sum(jnp.where(diag, pos_v[...].astype(F32), 0.0), axis=1, keepdims=True)
    pos_scr[...] = jnp.broadcast_to(pos_col, (n_seqs, PAIR))
    project(0, FIRST)
    pl.semaphore_wait(barrier, 2)

    lane_q = lax.broadcasted_iota(jnp.int32, (SUB, PAIR), 1)
    sub_q = lax.broadcasted_iota(jnp.int32, (SUB, PAIR), 0)
    head_mask = [lane_q < HEAD, lane_q >= HEAD]
    lane_p = lax.broadcasted_iota(jnp.int32, (SUB, cache_len), 1).astype(F32)
    stack = lambda x: jnp.concatenate([x] * (2 * GROUP), axis=0)

    tall = 2 * GROUP * SUB

    def attend(first_row, slot):
        scale = 1.0 / math.sqrt(HEAD)
        tiles_at = [pl.multiple_of(first_row + t * SUB, SUB) for t in range(BLOCK // SUB)]
        for t, base in enumerate(tiles_at):
            q_rows = []
            for g in range(GROUP):
                q_g = q_scr[g, pl.ds(base, SUB), :]
                for hd in range(2):
                    q_rows.append(jnp.where(head_mask[hd], q_g, 0.0))
            q_bd = jnp.concatenate([jnp.concatenate([jnp.where(sub_q == b, q, 0.0) for b in range(SUB)], axis=1)
                                    for q in q_rows], axis=0).astype(BF16)
            q_all = jnp.concatenate(q_rows, axis=0)
            at = slice(t * tall, (t + 1) * tall)
            n_scr[at, :] = jnp.broadcast_to(
                jnp.sum(q_all * stack(k_scr[pl.ds(base, SUB), :]), axis=1, keepdims=True) * scale, (tall, PAIR))
            s_scr[at, :] = jnp.dot(q_bd, k_buf[slot, t * SUB * PAIR:(t + 1) * SUB * PAIR, :],
                                   preferred_element_type=F32) * scale
        for t, base in enumerate(tiles_at):
            at = slice(t * tall, (t + 1) * tall)
            old = stack(lane_p < pos_scr[pl.ds(base, SUB), 0:1])
            scores = jnp.where(old, s_scr[at, :], -jnp.inf)
            score_new = n_scr[at, 0:1]
            top = jnp.maximum(jnp.max(scores, axis=1, keepdims=True), score_new)
            expd = jnp.exp(scores - top)
            exp_new = jnp.exp(score_new - top)
            inv = 1.0 / (jnp.sum(expd, axis=1, keepdims=True) + exp_new)
            p_scr[at, :] = (expd * inv).astype(BF16)
            n_scr[at, :] = jnp.broadcast_to((exp_new * inv).astype(BF16).astype(F32), (tall, PAIR))
        outs = []
        for t, base in enumerate(tiles_at):
            v_new = v_scr[pl.ds(base, SUB), :]
            mixed = lax.dot_general(p_scr[t * tall:(t + 1) * tall, :], v_buf[slot, t * SUB * PAIR:(t + 1) * SUB * PAIR, :],
                                    (((1,), (1,)), ((), ())), preferred_element_type=F32)
            pieces = []
            for g in range(GROUP):
                acc = None
                for hd in range(2):
                    lo = (g * 2 + hd) * SUB
                    piece = mixed[lo:lo + SUB, 0:PAIR]
                    for b in range(1, SUB):
                        piece = jnp.where(sub_q == b, mixed[lo:lo + SUB, b * PAIR:(b + 1) * PAIR], piece)
                    piece = piece + n_scr[t * tall + lo:t * tall + lo + SUB, :] * v_new
                    acc = piece if acc is None else jnp.where(head_mask[1], piece, acc)
                pieces.append(acc)
            outs.append(jnp.concatenate(pieces, axis=1))
        return jnp.concatenate(outs, axis=0).astype(BF16)

    def pair_step(p, carry):
        for slot in range(2):
            r = 2 * p + slot
            for c in cache_copies(r, slot):
                c.wait()
            o = attend(r * ROWS, slot)

            @pl.when(r + 2 < n_chunk)
            def _next(r=r, slot=slot):
                for c in cache_copies(r + 2, slot):
                    c.start()

            for i, c in enumerate(w_copies):
                if (2 * i // 3) % 2 == slot:
                    pl.when(r == 2 * i // 3)(c.start)

            @pl.when(r > 1)
            def _sum(r=r):
                sum_near(r - 1)

            if slot == 0:
                @pl.when(r == 0)
                def _w_out():
                    for c in wo_copies:
                        c.wait()

            part[other, chunk(r), :] = jnp.dot(o, wo_v[other], preferred_element_type=F32)
            near_copy(r).start()
            part[core, chunk(r), :] = jnp.dot(o, wo_v[core], preferred_element_type=F32)

            if slot == 0:
                @pl.when(r == 0)
                def _others():
                    normalize_in(FIRST, n_seqs)
                    project(FIRST, n_seqs)
                    sum_near(0)
        return carry

    lax.fori_loop(0, n_chunk // 2, pair_step, 0)
    sum_near(n_chunk - 1)
    for r in range(n_chunk):
        near_copy(r).wait_send()

    def sum_far_y(r):
        far_copy(r).wait_recv()
        total = resid_v[chunk(r), my_cols].astype(F32) + (mine[chunk(r), :] + far[chunk(r), :])
        full[core, chunk(r), :] = total.astype(BF16).astype(F32)
        back_copy(r).start()

    gain_row2 = gain_m[...].astype(F32).reshape(1, dim)
    outputs = [pltpu.make_async_copy(k_scr, knew_hbm, out_sem.at[2 * len(PARTS)]),
               pltpu.make_async_copy(v_scr, vnew_hbm, out_sem.at[2 * len(PARTS) + 1])]
    for c in outputs:
        c.start()
    for r in range(*PARTS[0]):
        sum_far_y(r)
    for m, (lo_chunk, hi_chunk) in enumerate(PARTS):
        chunks = range(lo_chunk, hi_chunk)
        n_rows = len(chunks) * ROWS

        def normalize(r):
            back_copy(r).wait_recv()
            x0 = full[0, chunk(r), :]
            x1 = full[1, chunk(r), :]
            mean_sq = (jnp.sum(x0 * x0, axis=1, keepdims=True)
                       + jnp.sum(x1 * x1, axis=1, keepdims=True)) * (1.0 / dim)
            inv = lax.rsqrt(mean_sq + EPS)
            at = pl.ds((r - chunks[0]) * ROWS, ROWS)
            h_scr[at, :half_dim] = (x0 * inv * gain_row2[:, :half_dim]).astype(BF16)
            h_scr[at, half_dim:] = (x1 * inv * gain_row2[:, half_dim:]).astype(BF16)

        for r in chunks:
            normalize(r)
        if m == 0:
            for c in w_copies[:2 * W_PARTS]:
                c.wait()

        def up_tile(n, carry, n_rows=n_rows):
            cols = pl.ds(pl.multiple_of(n * tile, tile), tile)
            h2 = h_scr[0:n_rows, :]
            gate = jnp.dot(h2, wg_v[:, cols], preferred_element_type=F32).astype(BF16).astype(F32)
            up = jnp.dot(h2, wu_v[:, cols], preferred_element_type=F32).astype(BF16).astype(F32)
            a_scr[0:n_rows, cols] = (gate * jax.nn.sigmoid(gate) * up).astype(BF16)
            return carry

        lax.fori_loop(0, ffn // tile, up_tile, 0)
        if m == 0:
            for c in w_copies[2 * W_PARTS:]:
                c.wait()
        part_at = pl.ds(lo_chunk * ROWS, n_rows)
        for s in (other, core):
            for n in range(n_tile):
                cols = pl.ds(pl.multiple_of(s * half_dim + n * tile, tile), tile)
                part[s, part_at, n * tile:(n + 1) * tile] = jnp.dot(
                    a_scr[0:n_rows, :], wd_v[:, cols], preferred_element_type=F32)
                if s is other:
                    near_copy_z(m, part_at, n).start()
        if m + 1 < len(PARTS):
            for r in range(*PARTS[m + 1]):
                sum_far_y(r)
        for n in range(n_tile):
            cols = slice(n * tile, (n + 1) * tile)
            near_copy_z(m, part_at, n).wait_recv()
            zsum[part_at, cols] = part[core, part_at, cols] + near[part_at, cols]
        if m == 0:
            for r in range(Z_IN):
                far_copy_z(r).start()
            part_at = pl.ds(Z_IN * ROWS, n_rows - Z_IN * ROWS)
        send_at = pl.ds(part_at.start - Z_IN * ROWS, part_at.size)
        sends = (pltpu.make_async_copy(full.at[core, part_at], x1_hbm.at[part_at], out_sem.at[2 * m]),
                 pltpu.make_async_copy(zsum.at[part_at], send_hbm.at[send_at], out_sem.at[2 * m + 1]))
        for c in sends:
            c.start()
        outputs += sends

    for r in range(Z_IN):
        far_copy_z(r).wait_recv()
        zfar[chunk(r), :] = full[core, chunk(r), :] + (zsum[chunk(r), :] + zfar[chunk(r), :])
    outputs.append(pltpu.make_async_copy(zfar, x1_hbm.at[pl.ds(0, Z_IN * ROWS)], out_sem.at[2 * len(PARTS) + 2]))
    outputs[-1].start()
    for c in outputs:
        c.wait()
    for m, (lo_chunk, hi_chunk) in enumerate(PARTS):
        for n in range(n_tile):
            near_copy_z(m, pl.ds(lo_chunk * ROWS, (hi_chunk - lo_chunk) * ROWS), n).wait_send()
    for r in range(n_chunk):
        back_copy(r).wait_send()
        far_copy(r).wait_send()
    for r in range(Z_IN):
        far_copy_z(r).wait_send()


def layer_call(resid_in, positions, kc, vc, gain_attn, w_query, w_key, w_value, w_out, gain_mlp, w_gate, w_up, w_down):
    n_seqs, dim = resid_in.shape
    half = dim // 2
    ffn = w_gate.shape[1]
    cache_len = kc.shape[1]
    n_chunk = n_seqs // ROWS
    hbm = pl.BlockSpec(memory_space=pl.ANY)
    sems = pltpu.SemaphoreType.DMA((2, n_chunk))
    freq = jnp.asarray(frequency_lanes())
    args = (positions.reshape(1, n_seqs), freq, resid_in, gain_attn, gain_mlp,
            w_query, w_key, w_value, kc, vc, w_out, w_gate, w_up, w_down)
    return pl.pallas_call(
        layer_kernel,
        out_shape=(jax.ShapeDtypeStruct((n_seqs, half), F32), jax.ShapeDtypeStruct((n_seqs - Z_IN * ROWS, half), F32),
                   jax.ShapeDtypeStruct((n_seqs, PAIR), F32), jax.ShapeDtypeStruct((n_seqs, PAIR), F32)),
        in_specs=[hbm] * len(args),
        out_specs=(hbm,) * 4,
        scratch_shapes=[
            pltpu.VMEM((1, n_seqs), jnp.int32), pltpu.VMEM(freq.shape, F32), pltpu.VMEM((n_seqs, dim), BF16),
            pltpu.VMEM((dim,), BF16), pltpu.VMEM((dim,), BF16),
            pltpu.VMEM(w_query.shape, BF16), pltpu.VMEM(w_key.shape, BF16), pltpu.VMEM(w_value.shape, BF16),
            pltpu.VMEM((2, BLOCK * PAIR, cache_len), BF16), pltpu.VMEM((2, BLOCK * PAIR, cache_len), BF16),
            pltpu.VMEM((2, w_out.shape[0], half), BF16), pltpu.VMEM(w_gate.shape, BF16),
            pltpu.VMEM(w_up.shape, BF16), pltpu.VMEM(w_down.shape, BF16),
            pltpu.VMEM((n_seqs, dim), BF16), pltpu.VMEM((max(hi - lo for lo, hi in PARTS) * ROWS, ffn), BF16),
            pltpu.VMEM((GROUP, n_seqs, PAIR), F32), pltpu.VMEM((n_seqs, PAIR), F32),
            pltpu.VMEM((n_seqs, PAIR), F32), pltpu.VMEM((n_seqs, PAIR), F32),
            pltpu.VMEM((2 * GROUP * BLOCK, cache_len), F32), pltpu.VMEM((2 * GROUP * BLOCK, cache_len), BF16),
            pltpu.VMEM((2 * GROUP * BLOCK, PAIR), F32),
            pltpu.VMEM((2, n_seqs, half), F32), pltpu.VMEM((n_seqs, half), F32),
            pltpu.VMEM((n_seqs, half), F32), pltpu.VMEM((n_seqs, half), F32),
            pltpu.VMEM((2, n_seqs, half), F32), pltpu.VMEM((n_seqs, half), F32),
            pltpu.VMEM((Z_IN * ROWS, half), F32),
            pltpu.SemaphoreType.DMA((8,)), pltpu.SemaphoreType.DMA((2, 2)), pltpu.SemaphoreType.DMA((16,)),
            pltpu.SemaphoreType.DMA((3 * W_PARTS,)), pltpu.SemaphoreType.DMA((3 + 2 * len(PARTS),)),
            sems, sems, sems, sems, sems, sems],
        compiler_params=pltpu.CompilerParams(collective_id=0, has_side_effects=True, vmem_limit_bytes=LAYER_VMEM),
        name="layer",
    )(*args)


def write_kernel(first_step, n_steps, pos_smem, knew_hbm, vnew_hbm, kc_hbm, vc_hbm, *refs):
    ko_hbm, vo_hbm, k_buf, v_buf, knew, vnew, new_sem, in_sem, out_sem = refs[-9:]
    cache_len = kc_hbm.shape[1]
    block = SEQS * PAIR
    width = PAIR
    lane = lax.broadcasted_iota(jnp.int32, (PAIR, width), 1)

    def copies(step):
        slot = lax.rem(step, SLOTS)
        at = pl.ds(pl.multiple_of((first_step + step) * block, block), block)
        return ((pltpu.make_async_copy(kc_hbm.at[at], k_buf.at[slot], in_sem.at[0, slot]),
                 pltpu.make_async_copy(vc_hbm.at[at], v_buf.at[slot], in_sem.at[1, slot])),
                (pltpu.make_async_copy(k_buf.at[slot], ko_hbm.at[at], out_sem.at[0, slot]),
                 pltpu.make_async_copy(v_buf.at[slot], vo_hbm.at[at], out_sem.at[1, slot])))

    for step in range(min(AHEAD, n_steps)):
        for c in copies(step)[0]:
            c.start()
    news = (pltpu.make_async_copy(knew_hbm, knew, new_sem.at[0]), pltpu.make_async_copy(vnew_hbm, vnew, new_sem.at[1]))
    for c in news:
        c.start()
    for c in news:
        c.wait()

    def body(step, carry):
        slot = lax.rem(step, SLOTS)
        ins, outs = copies(step)
        for c in ins:
            c.wait()

        @pl.when(step + AHEAD < n_steps)
        def _next():
            @pl.when(step + AHEAD >= SLOTS)
            def _free():
                for c in copies(step + AHEAD - SLOTS)[1]:
                    c.wait()
            for c in copies(step + AHEAD)[0]:
                c.start()

        for t in range(SEQS // SUB):
            base = pl.multiple_of((first_step + step) * SEQS + t * SUB, SUB)
            k_t = knew[pl.ds(base, SUB), :].T
            v_t = vnew[pl.ds(base, SUB), :].T
            for b in range(SUB):
                pos = pos_smem[base + b]
                lo = pl.multiple_of(pos // width * width, width)
                hit = lane == pos - lo
                at = pl.ds((t * SUB + b) * PAIR, PAIR)
                cols = pl.ds(lo, width)
                k_buf[slot, at, cols] = jnp.where(hit, k_t[:, b:b + 1], k_buf[slot, at, cols].astype(F32)).astype(BF16)
                v_buf[slot, at, cols] = jnp.where(hit, v_t[:, b:b + 1], v_buf[slot, at, cols].astype(F32)).astype(BF16)
        for c in outs:
            c.start()
        return carry

    lax.fori_loop(0, n_steps, body, 0)
    for step in range(max(0, n_steps - SLOTS), n_steps):
        for c in copies(step)[1]:
            c.wait()


def write_call(positions, knew, vnew, kc, vc, first_step, n_steps, prev=()):
    cache_len = kc.shape[1]
    hbm = pl.BlockSpec(memory_space=pl.ANY)
    buf = pltpu.VMEM((SLOTS, SEQS * PAIR, cache_len), BF16)
    return pl.pallas_call(
        functools.partial(write_kernel, first_step, n_steps),
        out_shape=(jax.ShapeDtypeStruct(kc.shape, BF16), jax.ShapeDtypeStruct(vc.shape, BF16)),
        in_specs=[pl.BlockSpec(memory_space=pltpu.SMEM)] + [hbm] * (4 + len(prev)),
        out_specs=(hbm, hbm),
        scratch_shapes=[buf, buf, pltpu.VMEM(knew.shape, F32), pltpu.VMEM(vnew.shape, F32), pltpu.SemaphoreType.DMA((2,)),
                        pltpu.SemaphoreType.DMA((2, SLOTS)), pltpu.SemaphoreType.DMA((2, SLOTS))],
        input_output_aliases={5 + i: i for i in range(len(prev))},
        compiler_params=pltpu.CompilerParams(vmem_limit_bytes=WRITE_VMEM),
        cost_estimate=pl.CostEstimate(flops=10 ** 10, bytes_accessed=4 * SEQS * PAIR * cache_len * 2 * n_steps,
                                      transcendentals=0),
        name="write",
    )(positions, knew, vnew, kc, vc, *prev)


def join_kernel(core_smem, mine_ref, other_ref, out_ref):
    half = mine_ref.shape[1]
    low = core_smem[0] == 0
    mine, other = mine_ref[...], other_ref[...]
    out_ref[:, :half] = jnp.where(low, mine, other).astype(BF16)
    out_ref[:, half:] = jnp.where(low, other, mine).astype(BF16)


def join_call(mine, other):
    n_seqs, half = mine.shape
    rows = 128
    one = pl.BlockSpec((rows, half), lambda i, c: (i, 0))
    return pl.pallas_call(
        join_kernel,
        out_shape=jax.ShapeDtypeStruct((n_seqs, 2 * half), BF16),
        grid_spec=pltpu.PrefetchScalarGridSpec(
            num_scalar_prefetch=1, grid=(n_seqs // rows,), in_specs=[one, one],
            out_specs=pl.BlockSpec((rows, 2 * half), lambda i, c: (i, 0))),
        compiler_params=pltpu.CompilerParams(dimension_semantics=("arbitrary",), vmem_limit_bytes=8 << 20),
        name="join",
    )((lax.axis_index('tp') % 2).reshape(1), mine, other)


FAR = [(0, 2), (1, 3), (2, 0), (3, 1)]
NEAR = [(0, 1), (1, 0), (2, 3), (3, 2)]


def solution(mesh):
    def layer_local(resid_in, positions, k_cache, v_cache, gain_attn, w_query, w_key, w_value,
                    w_out, gain_mlp, w_gate, w_up, w_down):
        n_seqs, cache_len, heads, dim = k_cache.shape
        flat = lambda c: jnp.transpose(c, (0, 2, 3, 1)).reshape(n_seqs * heads * dim, cache_len)
        back = lambda c: jnp.transpose(c.reshape(n_seqs, heads, dim, cache_len), (0, 3, 1, 2))
        kc, vc = flat(k_cache), flat(v_cache)
        x1, send, knew, vnew = layer_call(resid_in, positions, kc, vc, gain_attn, w_query, w_key, w_value,
                                                     w_out, gain_mlp, w_gate, w_up, w_down)
        far = lax.ppermute(send, 'tp', FAR)
        k_full, v_full = write_call(positions, knew, vnew, kc, vc, 0, n_seqs // SEQS)
        far, k_full, v_full = lax.optimization_barrier((far, k_full, v_full))
        total = x1 + jnp.pad(send + far, ((Z_IN * ROWS, 0), (0, 0)))
        total_other = lax.ppermute(total, 'tp', NEAR)
        resid_out = join_call(total, total_other)
        return resid_out, back(k_full), back(v_full)

    row_spec = P('dp', None)
    cache_spec = P('dp', None, 'tp', None)
    col_spec = P(None, 'tp')
    split_rows = P('tp', None)
    return jax.shard_map(layer_local, mesh=mesh,
                         in_specs=(row_spec, P('dp'), cache_spec, cache_spec, P(), col_spec, col_spec,
                                   col_spec, split_rows, P(), col_spec, col_spec, split_rows),
                         out_specs=(row_spec, cache_spec, cache_spec), check_vma=False)
```

```python
import functools
import math
import numpy as np
import jax
import jax.numpy as jnp
from jax import lax
from jax.experimental import pallas as pl
from jax.experimental.pallas import tpu as pltpu
from jax.sharding import PartitionSpec as P

EPS = 1e-5
ROPE_THETA = 500000.0
ROPE_FACTOR = 8.0
LOW_FACTOR = 1.0
HIGH_FACTOR = 4.0
ORIG_CTX = 8192.0
MESH = pl.DeviceIdType.MESH
F32 = jnp.float32
BF16 = jnp.bfloat16

HEAD = 64
PAIR = 128
GROUP = 4
SEQS = 16
SUB = 8
ROWS = 32
BLOCK = 32
Z_IN = 1
FIRST = 128
PARTS = ((0, 4), (4, 8))
LAYER_VMEM = 67043328
WRITE_VMEM = 56 << 20
W_PARTS = 4
SLOTS = 16
AHEAD = 16


def frequency_lanes():
    half = HEAD // 2
    exponents = np.arange(half, dtype=np.float32) * np.float32(2.0 / HEAD)
    inv_freq = (1.0 / np.power(np.float32(ROPE_THETA), exponents)).astype(np.float32)
    wavelen = (2.0 * math.pi) / inv_freq
    smooth = (ORIG_CTX / wavelen - LOW_FACTOR) / (HIGH_FACTOR - LOW_FACTOR)
    blended = (1.0 - smooth) * inv_freq / ROPE_FACTOR + smooth * inv_freq
    inv_freq = np.where(wavelen < ORIG_CTX / HIGH_FACTOR, inv_freq,
                        np.where(wavelen > ORIG_CTX / LOW_FACTOR, inv_freq / ROPE_FACTOR, blended))
    lanes = np.arange(PAIR)
    freq = inv_freq[lanes % half].astype(np.float32)
    sign = np.where(lanes % HEAD < half, -1.0, 1.0).astype(np.float32)
    return np.stack([freq, sign])


def layer_kernel(pos_hbm, freq_hbm, resid_hbm, gain_a_hbm, gain_m_hbm, wq_hbm, wk_hbm, wv_hbm, kc_hbm, vc_hbm,
                 wo_hbm, wg_hbm, wu_hbm, wd_hbm,
                 x1_hbm, send_hbm, knew_hbm, vnew_hbm,
                 pos_v, freq_v, resid_v, gain_a, gain_m, wq_v, wk_v, wv_v, k_buf, v_buf, wo_v, wg_v, wu_v, wd_v,
                 h_scr, a_scr, q_scr, k_scr, v_scr, pos_scr, s_scr, p_scr, n_scr,
                 part, near, mine, far, full, zsum, zfar,
                 in_sem, kv_sem, wo_sem, w_sem, out_sem,
                 near_send, near_recv, far_send, far_recv, back_send, back_recv):
    tp = lax.axis_index("tp")
    dp = lax.axis_index("dp")
    core = lax.rem(tp, 2)
    other = 1 - core
    sibling = tp + 1 - 2 * core
    partner = lax.rem(tp + 2, 4)
    n_seqs, dim = resid_v.shape
    cache_len = kc_hbm.shape[1]
    half_dim = dim // 2
    ffn = wg_v.shape[1]
    n_chunk = n_seqs // ROWS
    block = BLOCK * PAIR
    tile = 512
    n_tile = half_dim // tile

    inputs = [pltpu.make_async_copy(src, dst, in_sem.at[i]) for i, (src, dst) in enumerate((
        (resid_hbm, resid_v), (gain_a_hbm, gain_a), (wq_hbm, wq_v), (wk_hbm, wk_v), (wv_hbm, wv_v),
        (pos_hbm, pos_v), (freq_hbm, freq_v), (gain_m_hbm, gain_m)))]
    for c in inputs:
        c.start()

    def cache_copies(r, slot):
        at = pl.ds(pl.multiple_of(r * block, block), block)
        return (pltpu.make_async_copy(kc_hbm.at[at], k_buf.at[slot], kv_sem.at[0, slot]),
                pltpu.make_async_copy(vc_hbm.at[at], v_buf.at[slot], kv_sem.at[1, slot]))

    wo_copies = []
    for g in range(GROUP):
        for h in range(2):
            for s in range(2):
                wo_copies.append(pltpu.make_async_copy(
                    wo_hbm.at[pl.ds((h * GROUP + g) * HEAD, HEAD), pl.ds(s * half_dim, half_dim)],
                    wo_v.at[s, pl.ds((2 * g + h) * HEAD, HEAD), :], wo_sem.at[(2 * g + h) * 2 + s]))
    w_copies = []
    for src, dst in ((wg_hbm, wg_v), (wu_hbm, wu_v), (wd_hbm, wd_v)):
        rows = dst.shape[0] // W_PARTS
        for i in range(W_PARTS):
            at = pl.ds(i * rows, rows)
            w_copies.append(pltpu.make_async_copy(src.at[at], dst.at[at], w_sem.at[len(w_copies)]))

    barrier = pltpu.get_barrier_semaphore()
    for peer in (sibling, partner):
        pl.semaphore_signal(barrier, inc=1, device_id=(dp, peer), device_id_type=MESH)

    def remote(src, dst, sems, k, r, peer):
        return pltpu.make_async_remote_copy(src_ref=src, dst_ref=dst, send_sem=sems[0].at[k, r], recv_sem=sems[1].at[k, r],
                                            device_id=(dp, peer), device_id_type=MESH)

    def chunk(r):
        return pl.ds(pl.multiple_of(r * ROWS, ROWS), ROWS)

    def near_copy(r):
        return remote(part.at[other, chunk(r)], near.at[chunk(r)], (near_send, near_recv), 0, r, sibling)

    def near_copy_z(m, at, n):
        cols = pl.ds(n * tile, tile)
        return remote(part.at[other, at, cols], near.at[at, cols], (near_send, near_recv), 1, m * n_tile + n, sibling)

    def far_copy(r):
        return remote(mine.at[chunk(r)], far.at[chunk(r)], (far_send, far_recv), 0, r, partner)

    def back_copy(r):
        return remote(full.at[core, chunk(r)], full.at[core, chunk(r)], (back_send, back_recv), 0, r, sibling)

    def far_copy_z(r):
        return remote(zsum.at[chunk(r)], zfar.at[chunk(r)], (far_send, far_recv), 1, r, partner)

    def sum_near(r):
        near_copy(r).wait_recv()
        mine[chunk(r), :] = part[core, chunk(r), :] + near[chunk(r), :]
        far_copy(r).start()

    my_cols = pl.ds(pl.multiple_of(core * half_dim, half_dim), half_dim)
    other_cols = pl.ds(pl.multiple_of(other * half_dim, half_dim), half_dim)

    for c in inputs[:2]:
        c.wait()
    for c in cache_copies(0, 0):
        c.start()
    gain_row = gain_a[...].astype(F32).reshape(1, dim)

    def normalize_in(lo, hi):
        for i in range(lo, hi, FIRST):
            x = resid_v[i:i + FIRST, :].astype(F32)
            mean_sq = jnp.sum(x * x, axis=1, keepdims=True) * (1.0 / dim)
            h_scr[i:i + FIRST, :] = (x * lax.rsqrt(mean_sq + EPS) * gain_row).astype(BF16)

    def project(lo, hi):
        n = hi - lo
        at = slice(lo, hi)
        angles = pos_scr[at, :] * freq_v[0:1, :]
        cos_t = jnp.cos(angles)
        sin_t = jnp.sin(angles) * freq_v[1:2, :]
        lane = lax.broadcasted_iota(jnp.int32, (n, PAIR), 1)
        low = lane % HEAD < HEAD // 2
        first = lane < HEAD

        def rope(t):
            t = t.astype(BF16).astype(F32)
            swapped = jnp.where(low, pltpu.roll(t, PAIR - HEAD // 2, 1), pltpu.roll(t, HEAD // 2, 1))
            return (t * cos_t + swapped * sin_t).astype(BF16).astype(F32)

        h = h_scr[at, :]
        q_all = jnp.dot(h, wq_v[...], preferred_element_type=F32)
        tiles = [rope(q_all[:, t * PAIR:(t + 1) * PAIR]) for t in range(GROUP)]
        for g in range(GROUP):
            lower, upper = tiles[g // 2], tiles[2 + g // 2]
            if g % 2 == 0:
                upper = pltpu.roll(upper, HEAD, 1)
            else:
                lower = pltpu.roll(lower, HEAD, 1)
            q_scr[g, at, :] = jnp.where(first, lower, upper)
        k_scr[at, :] = rope(jnp.dot(h, wk_v[...], preferred_element_type=F32))
        v_scr[at, :] = jnp.dot(h, wv_v[...], preferred_element_type=F32).astype(BF16).astype(F32)

    normalize_in(0, FIRST)
    for c in inputs[2:]:
        c.wait()
    for c in (*wo_copies, *cache_copies(1, 1)):
        c.start()
    diag = (lax.broadcasted_iota(jnp.int32, (n_seqs, n_seqs), 0)
            == lax.broadcasted_iota(jnp.int32, (n_seqs, n_seqs), 1))
    pos_col = jnp.sum(jnp.where(diag, pos_v[...].astype(F32), 0.0), axis=1, keepdims=True)
    pos_scr[...] = jnp.broadcast_to(pos_col, (n_seqs, PAIR))
    project(0, FIRST)
    pl.semaphore_wait(barrier, 2)

    lane_q = lax.broadcasted_iota(jnp.int32, (SUB, PAIR), 1)
    sub_q = lax.broadcasted_iota(jnp.int32, (SUB, PAIR), 0)
    head_mask = [lane_q < HEAD, lane_q >= HEAD]
    lane_p = lax.broadcasted_iota(jnp.int32, (SUB, cache_len), 1).astype(F32)
    stack = lambda x: jnp.concatenate([x] * (2 * GROUP), axis=0)

    tall = 2 * GROUP * SUB

    def attend(first_row, slot):
        scale = 1.0 / math.sqrt(HEAD)
        tiles_at = [pl.multiple_of(first_row + t * SUB, SUB) for t in range(BLOCK // SUB)]
        for t, base in enumerate(tiles_at):
            q_rows = []
            for g in range(GROUP):
                q_g = q_scr[g, pl.ds(base, SUB), :]
                for hd in range(2):
                    q_rows.append(jnp.where(head_mask[hd], q_g, 0.0))
            q_bd = jnp.concatenate([jnp.concatenate([jnp.where(sub_q == b, q, 0.0) for b in range(SUB)], axis=1)
                                    for q in q_rows], axis=0).astype(BF16)
            q_all = jnp.concatenate(q_rows, axis=0)
            at = slice(t * tall, (t + 1) * tall)
            n_scr[at, :] = jnp.broadcast_to(
                jnp.sum(q_all * stack(k_scr[pl.ds(base, SUB), :]), axis=1, keepdims=True) * scale, (tall, PAIR))
            s_scr[at, :] = jnp.dot(q_bd, k_buf[slot, t * SUB * PAIR:(t + 1) * SUB * PAIR, :],
                                   preferred_element_type=F32) * scale
        for t, base in enumerate(tiles_at):
            at = slice(t * tall, (t + 1) * tall)
            old = stack(lane_p < pos_scr[pl.ds(base, SUB), 0:1])
            scores = jnp.where(old, s_scr[at, :], -jnp.inf)
            score_new = n_scr[at, 0:1]
            top = jnp.maximum(jnp.max(scores, axis=1, keepdims=True), score_new)
            expd = jnp.exp(scores - top)
            exp_new = jnp.exp(score_new - top)
            inv = 1.0 / (jnp.sum(expd, axis=1, keepdims=True) + exp_new)
            p_scr[at, :] = (expd * inv).astype(BF16)
            n_scr[at, :] = jnp.broadcast_to((exp_new * inv).astype(BF16).astype(F32), (tall, PAIR))
        outs = []
        for t, base in enumerate(tiles_at):
            v_new = v_scr[pl.ds(base, SUB), :]
            mixed = lax.dot_general(p_scr[t * tall:(t + 1) * tall, :], v_buf[slot, t * SUB * PAIR:(t + 1) * SUB * PAIR, :],
                                    (((1,), (1,)), ((), ())), preferred_element_type=F32)
            pieces = []
            for g in range(GROUP):
                acc = None
                for hd in range(2):
                    lo = (g * 2 + hd) * SUB
                    piece = mixed[lo:lo + SUB, 0:PAIR]
                    for b in range(1, SUB):
                        piece = jnp.where(sub_q == b, mixed[lo:lo + SUB, b * PAIR:(b + 1) * PAIR], piece)
                    piece = piece + n_scr[t * tall + lo:t * tall + lo + SUB, :] * v_new
                    acc = piece if acc is None else jnp.where(head_mask[1], piece, acc)
                pieces.append(acc)
            outs.append(jnp.concatenate(pieces, axis=1))
        return jnp.concatenate(outs, axis=0).astype(BF16)

    def pair_step(p, carry):
        for slot in range(2):
            r = 2 * p + slot
            for c in cache_copies(r, slot):
                c.wait()
            o = attend(r * ROWS, slot)

            @pl.when(r + 2 < n_chunk)
            def _next(r=r, slot=slot):
                for c in cache_copies(r + 2, slot):
                    c.start()

            for i, c in enumerate(w_copies):
                if (2 * i // 3) % 2 == slot:
                    pl.when(r == 2 * i // 3)(c.start)

            @pl.when(r > 1)
            def _sum(r=r):
                sum_near(r - 1)

            if slot == 0:
                @pl.when(r == 0)
                def _w_out():
                    for c in wo_copies:
                        c.wait()

            part[other, chunk(r), :] = jnp.dot(o, wo_v[other], preferred_element_type=F32)
            near_copy(r).start()
            part[core, chunk(r), :] = jnp.dot(o, wo_v[core], preferred_element_type=F32)

            if slot == 0:
                @pl.when(r == 0)
                def _others():
                    normalize_in(FIRST, n_seqs)
                    project(FIRST, n_seqs)
                    sum_near(0)
        return carry

    lax.fori_loop(0, n_chunk // 2, pair_step, 0)
    sum_near(n_chunk - 1)
    for r in range(n_chunk):
        near_copy(r).wait_send()

    def sum_far_y(r):
        far_copy(r).wait_recv()
        total = resid_v[chunk(r), my_cols].astype(F32) + (mine[chunk(r), :] + far[chunk(r), :])
        full[core, chunk(r), :] = total.astype(BF16).astype(F32)
        back_copy(r).start()

    gain_row2 = gain_m[...].astype(F32).reshape(1, dim)
    outputs = [pltpu.make_async_copy(k_scr, knew_hbm, out_sem.at[2 * len(PARTS)]),
               pltpu.make_async_copy(v_scr, vnew_hbm, out_sem.at[2 * len(PARTS) + 1])]
    for c in outputs:
        c.start()
    for r in range(*PARTS[0]):
        sum_far_y(r)
    for m, (lo_chunk, hi_chunk) in enumerate(PARTS):
        chunks = range(lo_chunk, hi_chunk)
        n_rows = len(chunks) * ROWS

        def normalize(r):
            back_copy(r).wait_recv()
            x0 = full[0, chunk(r), :]
            x1 = full[1, chunk(r), :]
            mean_sq = (jnp.sum(x0 * x0, axis=1, keepdims=True)
                       + jnp.sum(x1 * x1, axis=1, keepdims=True)) * (1.0 / dim)
            inv = lax.rsqrt(mean_sq + EPS)
            at = pl.ds((r - chunks[0]) * ROWS, ROWS)
            h_scr[at, :half_dim] = (x0 * inv * gain_row2[:, :half_dim]).astype(BF16)
            h_scr[at, half_dim:] = (x1 * inv * gain_row2[:, half_dim:]).astype(BF16)

        for r in chunks:
            normalize(r)
        x1_rows = chunks[0] * ROWS + (Z_IN * ROWS if m == 0 else 0)
        x1_at = pl.ds(x1_rows, chunks[-1] * ROWS + ROWS - x1_rows)
        outputs.append(pltpu.make_async_copy(full.at[core, x1_at], x1_hbm.at[x1_at], out_sem.at[2 * m]))
        outputs[-1].start()
        if m == 0:
            for c in w_copies[:2 * W_PARTS]:
                c.wait()

        def up_tile(n, carry, n_rows=n_rows):
            cols = pl.ds(pl.multiple_of(n * tile, tile), tile)
            h2 = h_scr[0:n_rows, :]
            gate = jnp.dot(h2, wg_v[:, cols], preferred_element_type=F32).astype(BF16).astype(F32)
            up = jnp.dot(h2, wu_v[:, cols], preferred_element_type=F32).astype(BF16).astype(F32)
            a_scr[0:n_rows, cols] = (gate * jax.nn.sigmoid(gate) * up).astype(BF16)
            return carry

        lax.fori_loop(0, ffn // tile, up_tile, 0)
        if m == 0:
            for c in w_copies[2 * W_PARTS:]:
                c.wait()
        part_at = pl.ds(lo_chunk * ROWS, n_rows)
        for s in (other, core):
            for n in range(n_tile):
                cols = pl.ds(pl.multiple_of(s * half_dim + n * tile, tile), tile)
                part[s, part_at, n * tile:(n + 1) * tile] = jnp.dot(
                    a_scr[0:n_rows, :], wd_v[:, cols], preferred_element_type=F32)
                if s is other:
                    near_copy_z(m, part_at, n).start()
        if m + 1 < len(PARTS):
            for r in range(*PARTS[m + 1]):
                sum_far_y(r)
        for n in range(n_tile):
            cols = slice(n * tile, (n + 1) * tile)
            near_copy_z(m, part_at, n).wait_recv()
            zsum[part_at, cols] = part[core, part_at, cols] + near[part_at, cols]
        if m == 0:
            for r in range(Z_IN):
                far_copy_z(r).start()
            part_at = pl.ds(Z_IN * ROWS, n_rows - Z_IN * ROWS)
        send_at = pl.ds(part_at.start - Z_IN * ROWS, part_at.size)
        sends = (pltpu.make_async_copy(zsum.at[part_at], send_hbm.at[send_at], out_sem.at[2 * m + 1]),)
        for c in sends:
            c.start()
        outputs += sends

    for r in range(Z_IN):
        far_copy_z(r).wait_recv()
        zfar[chunk(r), :] = full[core, chunk(r), :] + (zsum[chunk(r), :] + zfar[chunk(r), :])
    outputs.append(pltpu.make_async_copy(zfar, x1_hbm.at[pl.ds(0, Z_IN * ROWS)], out_sem.at[2 * len(PARTS) + 2]))
    outputs[-1].start()
    for c in outputs:
        c.wait()
    for m, (lo_chunk, hi_chunk) in enumerate(PARTS):
        for n in range(n_tile):
            near_copy_z(m, pl.ds(lo_chunk * ROWS, (hi_chunk - lo_chunk) * ROWS), n).wait_send()
    for r in range(n_chunk):
        back_copy(r).wait_send()
        far_copy(r).wait_send()
    for r in range(Z_IN):
        far_copy_z(r).wait_send()


def layer_call(resid_in, positions, kc, vc, gain_attn, w_query, w_key, w_value, w_out, gain_mlp, w_gate, w_up, w_down):
    n_seqs, dim = resid_in.shape
    half = dim // 2
    ffn = w_gate.shape[1]
    cache_len = kc.shape[1]
    n_chunk = n_seqs // ROWS
    hbm = pl.BlockSpec(memory_space=pl.ANY)
    sems = pltpu.SemaphoreType.DMA((2, n_chunk))
    freq = jnp.asarray(frequency_lanes())
    args = (positions.reshape(1, n_seqs), freq, resid_in, gain_attn, gain_mlp,
            w_query, w_key, w_value, kc, vc, w_out, w_gate, w_up, w_down)
    return pl.pallas_call(
        layer_kernel,
        out_shape=(jax.ShapeDtypeStruct((n_seqs, half), F32), jax.ShapeDtypeStruct((n_seqs - Z_IN * ROWS, half), F32),
                   jax.ShapeDtypeStruct((n_seqs, PAIR), F32), jax.ShapeDtypeStruct((n_seqs, PAIR), F32)),
        in_specs=[hbm] * len(args),
        out_specs=(hbm,) * 4,
        scratch_shapes=[
            pltpu.VMEM((1, n_seqs), jnp.int32), pltpu.VMEM(freq.shape, F32), pltpu.VMEM((n_seqs, dim), BF16),
            pltpu.VMEM((dim,), BF16), pltpu.VMEM((dim,), BF16),
            pltpu.VMEM(w_query.shape, BF16), pltpu.VMEM(w_key.shape, BF16), pltpu.VMEM(w_value.shape, BF16),
            pltpu.VMEM((2, BLOCK * PAIR, cache_len), BF16), pltpu.VMEM((2, BLOCK * PAIR, cache_len), BF16),
            pltpu.VMEM((2, w_out.shape[0], half), BF16), pltpu.VMEM(w_gate.shape, BF16),
            pltpu.VMEM(w_up.shape, BF16), pltpu.VMEM(w_down.shape, BF16),
            pltpu.VMEM((n_seqs, dim), BF16), pltpu.VMEM((max(hi - lo for lo, hi in PARTS) * ROWS, ffn), BF16),
            pltpu.VMEM((GROUP, n_seqs, PAIR), F32), pltpu.VMEM((n_seqs, PAIR), F32),
            pltpu.VMEM((n_seqs, PAIR), F32), pltpu.VMEM((n_seqs, PAIR), F32),
            pltpu.VMEM((2 * GROUP * BLOCK, cache_len), F32), pltpu.VMEM((2 * GROUP * BLOCK, cache_len), BF16),
            pltpu.VMEM((2 * GROUP * BLOCK, PAIR), F32),
            pltpu.VMEM((2, n_seqs, half), F32), pltpu.VMEM((n_seqs, half), F32),
            pltpu.VMEM((n_seqs, half), F32), pltpu.VMEM((n_seqs, half), F32),
            pltpu.VMEM((2, n_seqs, half), F32), pltpu.VMEM((n_seqs, half), F32),
            pltpu.VMEM((Z_IN * ROWS, half), F32),
            pltpu.SemaphoreType.DMA((8,)), pltpu.SemaphoreType.DMA((2, 2)), pltpu.SemaphoreType.DMA((16,)),
            pltpu.SemaphoreType.DMA((3 * W_PARTS,)), pltpu.SemaphoreType.DMA((3 + 2 * len(PARTS),)),
            sems, sems, sems, sems, sems, sems],
        compiler_params=pltpu.CompilerParams(collective_id=0, has_side_effects=True, vmem_limit_bytes=LAYER_VMEM),
        name="layer",
    )(*args)


def write_kernel(first_step, n_steps, pos_smem, knew_hbm, vnew_hbm, kc_hbm, vc_hbm, *refs):
    ko_hbm, vo_hbm, k_buf, v_buf, knew, vnew, new_sem, in_sem, out_sem = refs[-9:]
    cache_len = kc_hbm.shape[1]
    block = SEQS * PAIR
    width = PAIR
    lane = lax.broadcasted_iota(jnp.int32, (PAIR, width), 1)

    def copies(step):
        slot = lax.rem(step, SLOTS)
        at = pl.ds(pl.multiple_of((first_step + step) * block, block), block)
        return ((pltpu.make_async_copy(kc_hbm.at[at], k_buf.at[slot], in_sem.at[0, slot]),
                 pltpu.make_async_copy(vc_hbm.at[at], v_buf.at[slot], in_sem.at[1, slot])),
                (pltpu.make_async_copy(k_buf.at[slot], ko_hbm.at[at], out_sem.at[0, slot]),
                 pltpu.make_async_copy(v_buf.at[slot], vo_hbm.at[at], out_sem.at[1, slot])))

    for step in range(min(AHEAD, n_steps)):
        for c in copies(step)[0]:
            c.start()
    news = (pltpu.make_async_copy(knew_hbm, knew, new_sem.at[0]), pltpu.make_async_copy(vnew_hbm, vnew, new_sem.at[1]))
    for c in news:
        c.start()
    for c in news:
        c.wait()

    def body(step, carry):
        slot = lax.rem(step, SLOTS)
        ins, outs = copies(step)
        for c in ins:
            c.wait()

        @pl.when(step + AHEAD < n_steps)
        def _next():
            @pl.when(step + AHEAD >= SLOTS)
            def _free():
                for c in copies(step + AHEAD - SLOTS)[1]:
                    c.wait()
            for c in copies(step + AHEAD)[0]:
                c.start()

        for t in range(SEQS // SUB):
            base = pl.multiple_of((first_step + step) * SEQS + t * SUB, SUB)
            k_t = knew[pl.ds(base, SUB), :].T
            v_t = vnew[pl.ds(base, SUB), :].T
            for b in range(SUB):
                pos = pos_smem[base + b]
                lo = pl.multiple_of(pos // width * width, width)
                hit = lane == pos - lo
                at = pl.ds((t * SUB + b) * PAIR, PAIR)
                cols = pl.ds(lo, width)
                k_buf[slot, at, cols] = jnp.where(hit, k_t[:, b:b + 1], k_buf[slot, at, cols].astype(F32)).astype(BF16)
                v_buf[slot, at, cols] = jnp.where(hit, v_t[:, b:b + 1], v_buf[slot, at, cols].astype(F32)).astype(BF16)
        for c in outs:
            c.start()
        return carry

    lax.fori_loop(0, n_steps, body, 0)
    for step in range(max(0, n_steps - SLOTS), n_steps):
        for c in copies(step)[1]:
            c.wait()


def write_call(positions, knew, vnew, kc, vc, first_step, n_steps, prev=()):
    cache_len = kc.shape[1]
    hbm = pl.BlockSpec(memory_space=pl.ANY)
    buf = pltpu.VMEM((SLOTS, SEQS * PAIR, cache_len), BF16)
    return pl.pallas_call(
        functools.partial(write_kernel, first_step, n_steps),
        out_shape=(jax.ShapeDtypeStruct(kc.shape, BF16), jax.ShapeDtypeStruct(vc.shape, BF16)),
        in_specs=[pl.BlockSpec(memory_space=pltpu.SMEM)] + [hbm] * (4 + len(prev)),
        out_specs=(hbm, hbm),
        scratch_shapes=[buf, buf, pltpu.VMEM(knew.shape, F32), pltpu.VMEM(vnew.shape, F32), pltpu.SemaphoreType.DMA((2,)),
                        pltpu.SemaphoreType.DMA((2, SLOTS)), pltpu.SemaphoreType.DMA((2, SLOTS))],
        input_output_aliases={5 + i: i for i in range(len(prev))},
        compiler_params=pltpu.CompilerParams(vmem_limit_bytes=WRITE_VMEM),
        cost_estimate=pl.CostEstimate(flops=10 ** 10, bytes_accessed=4 * SEQS * PAIR * cache_len * 2 * n_steps,
                                      transcendentals=0),
        name="write",
    )(positions, knew, vnew, kc, vc, *prev)


def join_kernel(core_smem, mine_ref, other_ref, out_ref):
    half = mine_ref.shape[1]
    low = core_smem[0] == 0
    mine, other = mine_ref[...], other_ref[...]
    out_ref[:, :half] = jnp.where(low, mine, other).astype(BF16)
    out_ref[:, half:] = jnp.where(low, other, mine).astype(BF16)


def join_call(mine, other):
    n_seqs, half = mine.shape
    rows = 128
    one = pl.BlockSpec((rows, half), lambda i, c: (i, 0))
    return pl.pallas_call(
        join_kernel,
        out_shape=jax.ShapeDtypeStruct((n_seqs, 2 * half), BF16),
        grid_spec=pltpu.PrefetchScalarGridSpec(
            num_scalar_prefetch=1, grid=(n_seqs // rows,), in_specs=[one, one],
            out_specs=pl.BlockSpec((rows, 2 * half), lambda i, c: (i, 0))),
        compiler_params=pltpu.CompilerParams(dimension_semantics=("arbitrary",), vmem_limit_bytes=8 << 20),
        name="join",
    )((lax.axis_index('tp') % 2).reshape(1), mine, other)


FAR = [(0, 2), (1, 3), (2, 0), (3, 1)]
NEAR = [(0, 1), (1, 0), (2, 3), (3, 2)]


def solution(mesh):
    def layer_local(resid_in, positions, k_cache, v_cache, gain_attn, w_query, w_key, w_value,
                    w_out, gain_mlp, w_gate, w_up, w_down):
        n_seqs, cache_len, heads, dim = k_cache.shape
        flat = lambda c: jnp.transpose(c, (0, 2, 3, 1)).reshape(n_seqs * heads * dim, cache_len)
        back = lambda c: jnp.transpose(c.reshape(n_seqs, heads, dim, cache_len), (0, 3, 1, 2))
        kc, vc = flat(k_cache), flat(v_cache)
        x1, send, knew, vnew = layer_call(resid_in, positions, kc, vc, gain_attn, w_query, w_key, w_value,
                                                     w_out, gain_mlp, w_gate, w_up, w_down)
        far = lax.ppermute(send, 'tp', FAR)
        k_full, v_full = write_call(positions, knew, vnew, kc, vc, 0, n_seqs // SEQS)
        far, k_full, v_full = lax.optimization_barrier((far, k_full, v_full))
        total = x1 + jnp.pad(send + far, ((Z_IN * ROWS, 0), (0, 0)))
        total_other = lax.ppermute(total, 'tp', NEAR)
        resid_out = join_call(total, total_other)
        return resid_out, back(k_full), back(v_full)

    row_spec = P('dp', None)
    cache_spec = P('dp', None, 'tp', None)
    col_spec = P(None, 'tp')
    split_rows = P('tp', None)
    return jax.shard_map(layer_local, mesh=mesh,
                         in_specs=(row_spec, P('dp'), cache_spec, cache_spec, P(), col_spec, col_spec,
                                   col_spec, split_rows, P(), col_spec, col_spec, split_rows),
                         out_specs=(row_spec, cache_spec, cache_spec), check_vma=False)
```
